512 devices in a mesh: dp: 16 (over y_lo, x), space: 32 (over z, y_hi, core).
Axes of the slice: x: 4, y: 8 (y_hi: 2, y_lo: 4; y = y_hi * 4 + y_lo), z: 8, core: 2. Of those that a mesh axis runs over, the one named last changes fastest.
Arguments:
- fields: bfloat16 [16, 100, 131072], P('dp', None, 'space'), may hold values from -6 to 6
- cell_index: int32 [1024, 128], P('space'), may hold values from 0 to 6143
- interp_weight: bfloat16 [1024, 16, 128], P('space'), may hold values from 0 to 2, as said below
- w_in: bfloat16 [100, 1024], replicated, may hold values from -0.625 to 0.625
- ln_gain: float32 [1024], replicated, may hold values from 0.5 to 1.5
- w_qkv: bfloat16 [1024, 3072], P('dp'), may hold values from -0.1875 to 0.1875
- w_out: bfloat16 [1024, 1024], P('dp'), may hold values from -3 to 3
Outputs:
- latent: bfloat16 [16, 16384, 1024], P('dp', 'space')
- update: bfloat16 [16, 16384, 1024], P('dp', 'space')
The draws below stay inside these ranges and needn't reach their ends.
Inputs may be any that keep to these rules, and one draw needn't show every extreme that they name: `interp_weight`: in each block the slots from some count on carry zero weight for all its 16 nodes; that count lies between 48 and 128. `cell_index`: indexes a shard's 4096 cells extended by 1024 cells of each neighbouring shard, lower neighbour first.
All inputs are finite; a program needn't handle non-finite values.
Results may differ from the reference program's by a relative error of at most 0.0068.
Values may be sent and summed in bfloat16 or wider, within the bound.
No kernel may reach another device: no remote copies, remote signals or barrier semaphores. Data moves between devices by JAX's collectives and lax.ppermute only.
A program may use at most 128 MiB of HBM per device.

```python
import math
import jax
import jax.numpy as jnp
from jax import lax

D = 1024
HEADS = 16
CH = 100
NBLK = 16
SLOTS = 128
NODE_DEV = 512
CELL_DEV = 4096
HEAD_SIZE = 64
HALO_C = 1024
HALO_N = 256
BLK_DEV = 32
SAMPLES = 16
NODES = 16384
CELLS = 131072
BLOCKS = 1024
N_SPACE = 32


def draw_interp_weight(key, part):
    count_key, chosen_key, magnitude_key = jax.random.split(key, 3)
    full_shape = (BLOCKS, NBLK, SLOTS)
    live_count = jax.random.randint(count_key, (BLOCKS, 1, 1), 3 * SLOTS // 8, SLOTS + 1)
    slot_index = lax.broadcasted_iota(jnp.int32, full_shape, 2)
    chosen = jax.random.randint(chosen_key, full_shape, 0, 2)
    kept_mask = (slot_index < live_count) & (chosen == 0)
    magnitude = jax.random.uniform(magnitude_key, full_shape, jnp.float32, 0.0, 1.0)
    return jnp.where(kept_mask, magnitude, 0.0).astype(jnp.float32).astype(jnp.bfloat16)


def plant(array, rng, low, largest):
    spot = [jax.random.randint(jax.random.fold_in(rng, axis), (), 0, length) for axis, length in enumerate(array.shape)]
    longest = array.shape.index(max(array.shape))
    beside = spot[:longest] + [(spot[longest] + 1) % array.shape[longest]] + spot[longest + 1:]
    return array.at[tuple(spot)].set(low).at[tuple(beside)].set(largest)


def block_scale(stream_key, dims, shards, least, top_value):
    level, own = 1.0, jax.random.fold_in(stream_key, 6)
    for axis_at, shards_of in shards:
        heights = jnp.exp(jax.random.uniform(jax.random.fold_in(own, axis_at), (shards_of,), jnp.float32, least / len(shards), top_value / len(shards)))
        level = level * jnp.repeat(heights, dims[axis_at] // shards_of).reshape([-1 if axis == axis_at else 1 for axis in range(len(dims))])
    return level


def bell_draw(key, extent, width, bound, shards=(), kind=jnp.bfloat16):
    entries = width * jax.random.normal(key, extent, jnp.float32)
    if shards:
        entries = entries * block_scale(key, extent, shards, -0.22, 0.18)
    return jnp.clip(entries, -bound, bound).astype(kind)


def setup_inputs(seed: int = 0) -> dict:
    seeds = jax.random.split(jax.random.key(seed), 8)
    fields = bell_draw(seeds[0], (SAMPLES, CH, CELLS), 1.0, 6.0, ((0, 16), (2, 32)))
    cell_index = plant(jax.random.randint(seeds[1], (BLOCKS, SLOTS), 0, CELL_DEV + 2 * HALO_C), jax.random.fold_in(seeds[1], 1), 0, (CELL_DEV + 2 * HALO_C) - 1).astype(jnp.int32)
    interp_weight = draw_interp_weight(jax.random.fold_in(seeds[7], 71), 0)
    w_in = bell_draw(seeds[3], (CH, D), CH ** -0.5, 0.625)
    ln_gain = jnp.clip(1.0 + 0.1 * jax.random.normal(seeds[4], (D,), jnp.float32), 0.5, 1.5)
    w_qkv = bell_draw(seeds[5], (D, 3 * D), D ** -0.5, 0.1875, ((0, 16),))
    w_out = bell_draw(seeds[6], (D, D), (max(D // 256, 1)) ** -0.5, 3.0, ((0, 16),))
    return {"fields": fields, "cell_index": cell_index, "interp_weight": interp_weight, "w_in": w_in, "ln_gain": ln_gain, "w_qkv": w_qkv, "w_out": w_out}


def unit_heads(projected):
    head_rows = projected.reshape(projected.shape[0], HEADS, HEAD_SIZE)
    scale_rows = jnp.sqrt(lax.optimization_barrier(jnp.mean(head_rows * head_rows, axis=-1, keepdims=True)) + 1e-06)
    return (head_rows / scale_rows).astype(jnp.bfloat16)

def one_sample(grid_field, cell_index, interp_weight, w_in, ln_gain, w_qkv, w_out):
    owner_shard = jnp.arange(BLOCKS, dtype=jnp.int32) // BLK_DEV
    source = (owner_shard[:, None] * CELL_DEV - HALO_C + cell_index) % CELLS
    picked = jnp.take(grid_field, source.astype(jnp.int32), axis=1).astype(jnp.float32)
    encoded = jnp.einsum('cbs,bns->bnc', picked, interp_weight.astype(jnp.float32))
    encoded = encoded.reshape(NODES, CH).astype(jnp.bfloat16)
    embedded = jnp.dot(encoded, w_in, preferred_element_type=jnp.float32)
    average = lax.optimization_barrier(jnp.mean(embedded, axis=1, keepdims=True))
    centered = embedded - average
    spread = lax.optimization_barrier(jnp.mean(centered * centered, axis=1, keepdims=True))
    normed = (centered / jnp.sqrt(spread + 1e-05) * ln_gain).astype(jnp.bfloat16)
    projected = jnp.dot(normed, w_qkv, preferred_element_type=jnp.float32)
    queries = unit_heads(projected[:, :D])
    keys_all = unit_heads(projected[:, D:2 * D])
    values_all = projected[:, 2 * D:].reshape(NODES, HEADS, HEAD_SIZE).astype(jnp.bfloat16)
    wrapped_keys = jnp.concatenate([keys_all[NODES - HALO_N:], keys_all, keys_all[:HALO_N]], axis=0)
    wrapped_values = jnp.concatenate([values_all[NODES - HALO_N:], values_all, values_all[:HALO_N]], axis=0)

    def attend(shard_index):
        first_row = shard_index * NODE_DEV
        query_rows = lax.dynamic_slice_in_dim(queries, first_row, NODE_DEV, 0).astype(jnp.float32)
        key_rows = lax.dynamic_slice_in_dim(wrapped_keys, first_row, NODE_DEV + 2 * HALO_N, 0).astype(jnp.float32)
        value_rows = lax.dynamic_slice_in_dim(wrapped_values, first_row, NODE_DEV + 2 * HALO_N, 0).astype(jnp.float32)
        scores = jnp.einsum('qhd,khd->hqk', query_rows, key_rows) / math.sqrt(HEAD_SIZE)
        weights = jnp.exp(scores)
        probs = (weights / lax.optimization_barrier(jnp.sum(weights, axis=2, keepdims=True))).astype(jnp.bfloat16)
        mixed_rows = jnp.einsum('hqk,khd->qhd', probs.astype(jnp.float32), value_rows)
        return mixed_rows.astype(jnp.bfloat16).reshape(NODE_DEV, D)
    attended = lax.map(attend, jnp.arange(N_SPACE, dtype=jnp.int32)).reshape(NODES, D)
    update = jnp.dot(attended, w_out, preferred_element_type=jnp.float32).astype(jnp.bfloat16)
    return (embedded.astype(jnp.bfloat16), update)

def reference(fields, cell_index, interp_weight, w_in, ln_gain, w_qkv, w_out):

    def per_sample(grid_field):
        return one_sample(grid_field, cell_index, interp_weight, w_in, ln_gain, w_qkv, w_out)
    latent, update = lax.map(per_sample, fields)
    return (latent, update)
```

```python
import functools
import math

import jax
import jax.numpy as jnp
from jax import lax
from jax.experimental import pallas as pl
from jax.experimental.pallas import tpu as pltpu
from jax.sharding import PartitionSpec as P


HEADS = 16
BF, F32 = jnp.bfloat16, jnp.float32
AXES = ("dp", "space")
REL = (0, -1, 1, 2)


def coords(dp, s):
    return dp % 4, (s // 2 % 2) * 4 + dp // 4, s // 4, s % 2


def index(x, y, z, c):
    x, y, z = x % 4, y % 8, z % 8
    return ((y % 4) * 4 + x) * 32 + z * 4 + (y // 4) * 2 + c


def send(array, move):
    pairs = [
        (dp * 32 + s, index(*move(*coords(dp, s)))) for dp in range(16) for s in range(32)
    ]
    return lax.ppermute(array, AXES, pairs)


def along(first, step):
    def move(x, y, z, c):
        return (x + step, y, z, c) if (c == 0) == first else (x, y + step, z, c)

    return move


def swap(array):
    return send(array, lambda x, y, z, c: (x, y, z, 1 - c))


def ring(array, move):
    return lax.ppermute(array, "space", [(s, move(s) % 32) for s in range(32)])


def call(kernel, outs, scratch, flops, limit, n_in, name):
    return pl.pallas_call(
        kernel,
        out_shape=[jax.ShapeDtypeStruct(s, d) for s, d in outs],
        in_specs=[pl.BlockSpec(memory_space=pltpu.SMEM)]
        + [pl.BlockSpec(memory_space=pltpu.VMEM)] * n_in,
        out_specs=[pl.BlockSpec(memory_space=pltpu.VMEM)] * len(outs),
        scratch_shapes=[pltpu.VMEM(s, d) for s, d in scratch],
        compiler_params=pltpu.CompilerParams(vmem_limit_bytes=limit << 20),
        cost_estimate=pl.CostEstimate(flops=flops, bytes_accessed=1 << 20, transcendentals=0),
        name=name,
    )


def dot(a, b):
    return jnp.dot(a, b, preferred_element_type=F32)


def embed_kernel(where, own, partner, near, far, w_in, gain, normed, latent, window):
    core = where[0]

    def put(start, piece):
        window[pl.ds(pl.multiple_of(start, 256), piece.shape[0]), :] = piece[...]

    put(256 + core * 512, own)
    put(768 - core * 512, partner)
    put(core * 1280, near)
    put(1280 - core * 1280, far)

    def tile(i, carry):
        rows = pl.ds(pl.multiple_of(i * 128, 128), 128)
        embedded = dot(window[rows, :], w_in[...])
        average = jnp.mean(embedded, axis=1, keepdims=True)
        centered = embedded - average
        spread = jnp.mean(centered * centered, axis=1, keepdims=True)
        normed[rows, :] = (centered * lax.rsqrt(spread + 1e-05) * gain[...]).astype(BF)
        mine = i - 2 - 4 * core

        @pl.when((mine >= 0) & (mine < 4))
        def _():
            latent[pl.ds(pl.multiple_of(mine * 128, 128), 128), :] = embedded.astype(BF)

        return carry

    lax.fori_loop(0, 12, tile, 0)


def project_kernel(where, normed, own, before, after, half_a, half_b, q, k, v, out_cols, weights):
    core, x, y = where[0], where[1], where[2]

    def put(piece, row, a, b):
        dx = jnp.where(core == 0, a, b)
        dy = jnp.where(core == 0, b, a)
        block = lax.rem(y + dy + 4, 4) * 4 + lax.rem(x + dx + 4, 4)
        rows = pl.ds(pl.multiple_of(block * 64, 64), 64)
        weights[rows, :] = piece[row : row + 64, :1536]
        out_cols[rows, :] = piece[row : row + 64, 1536:]

    for i, a in enumerate(REL):
        put(own, i * 64, a, 0)
        put(before, i * 64, a, -1)
        put(after, i * 64, a, 1)
        put(half_a if i < 2 else half_b, (i % 2) * 64, a, 2)

    same = lax.broadcasted_iota(jnp.int32, (256, 256), 0) // 64 == (
        lax.broadcasted_iota(jnp.int32, (256, 256), 1) // 64
    )
    ones = jnp.where(same, 1.0, 0.0).astype(BF)

    def unit_heads(rows, ref, at):
        for h in range(2):
            part = rows[:, h * 256 : (h + 1) * 256]
            squares = dot((part * part).astype(BF), ones)
            unit = (part * lax.rsqrt(squares * (1.0 / 64) + 1e-06)).astype(BF)
            ref[2 * h, at, :] = unit[:, :128]
            ref[2 * h + 1, at, :] = unit[:, 128:]

    def tile(i, carry):
        at = pl.ds(pl.multiple_of(i * 256, 256), 256)
        rows = normed[at, :]
        unit_heads(dot(rows, weights[:, 512:1024]), k, at)
        values = dot(rows, weights[:, 1024:1536]).astype(BF)
        for p in range(4):
            v[p, at, :] = values[:, p * 128 : (p + 1) * 128]

        @pl.when((i >= 1) & (i < 5))
        def _():
            to = pl.ds(pl.multiple_of((i - 1) * 256, 256), 256)
            unit_heads(dot(rows, weights[:, :512]), q, to)

        return carry

    lax.fori_loop(0, 6, tile, 0)


def attend_kernel(shard, q, k, v, out):
    scale = math.log2(math.e) / 8.0
    low = lax.broadcasted_iota(jnp.int32, (256, 128), 1) < 64

    def tile(i, carry):
        p, part = lax.div(i, 2), lax.rem(i, 2)
        start = pl.multiple_of(shard[0] * 512, 512)
        query = q[p, pl.ds(pl.multiple_of(start + part * 256, 256), 256), :]
        keys = k[p, pl.ds(start, 1024), :]
        values = v[p, pl.ds(start, 1024), :]
        wide = jnp.concatenate([values, jnp.ones((1024, 128), BF)], axis=1)
        zero = jnp.zeros_like(query)
        mixed = []
        for head in (jnp.where(low, query, zero), jnp.where(low, zero, query)):
            scores = lax.dot_general(
                head, keys, (((1,), (1,)), ((), ())), preferred_element_type=F32
            )
            both = dot(jnp.exp2(scores * scale).astype(BF), wide)
            mixed.append(both[:, :128] / both[:, 128:])
        out[p, pl.ds(pl.multiple_of(part * 256, 256), 256), :] = jnp.where(
            low, mixed[0], mixed[1]
        ).astype(BF)
        return carry

    lax.fori_loop(0, 8, tile, 0)


def out_kernel(where, mine, theirs, my_cols, their_cols, update):
    core = where[0]
    join = lambda ref: jnp.concatenate([ref[p] for p in range(4)], axis=1)
    here, there = join(mine), join(theirs)
    near = pl.ds(pl.multiple_of(core * 512, 512), 512)
    far = pl.ds(pl.multiple_of(512 - core * 512, 512), 512)
    for cols, at in ((my_cols, near), (their_cols, far)):
        update[:, at] = (dot(here, cols[near, :]) + dot(there, cols[far, :])).astype(BF)


def shards(fields, cell_index, interp_weight, w_in, ln_gain, w_qkv, w_out):
    dp, space = lax.axis_index("dp"), lax.axis_index("space")
    core = lax.rem(space, 2)
    slot = lax.iota(jnp.int32, 4)
    where = jnp.where(slot == 0, core, jnp.where(slot == 1, lax.rem(dp, 4), lax.div(dp, 4)))

    grid_field = fields[0]
    before = ring(grid_field[:, -1024:], lambda s: s + 1)
    after = ring(grid_field[:, :1024], lambda s: s - 1)

    even = core == 0
    both = jnp.concatenate([w_qkv, w_out], axis=1).reshape(64, 4, 1024)
    block = jnp.where(even, both[:, :, :512], both[:, :, 512:]).reshape(64, 2048)
    line = [block] + [send(block, along(True, step)) for step in (1, -1, 2)]
    group = jnp.concatenate(line, axis=0)
    from_before = send(group, along(False, 1))
    from_after = send(group, along(False, -1))
    half_a = send(from_before[:128], along(False, 1))
    half_b = send(from_after[128:], along(False, -1))

    extended = jnp.concatenate([before, grid_field, after], axis=1)
    picked = jnp.take(extended, cell_index, axis=1)
    encoded = jnp.einsum("cbs,bns->bnc", picked, interp_weight, preferred_element_type=F32)
    encoded = jnp.pad(encoded.reshape(512, 100).astype(BF), ((0, 0), (0, 28)))
    edge = jnp.where(even, encoded[:256], encoded[256:])
    partner = swap(encoded)
    near = ring(edge, lambda s: s + 1 if s % 2 else s - 1)
    far = ring(edge, lambda s: s + 2 if s % 2 else s - 2)

    normed, latent = call(
        embed_kernel,
        [((1536, 1024), BF), ((512, 1024), BF)],
        [((1536, 128), BF)],
        4_000_000_000,
        16,
        6,
        "embed",
    )(where, encoded, partner, near, far, jnp.pad(w_in, ((0, 28), (0, 0))), ln_gain[None])
    q, k, v, my_cols = call(
        project_kernel,
        [((4, 1024, 128), BF), ((4, 1536, 128), BF), ((4, 1536, 128), BF), ((1024, 512), BF)],
        [((1024, 1536), BF)],
        8_000_000_000,
        32,
        6,
        "project",
    )(where, normed, group, from_before, from_after, half_a, half_b)
    their_cols = swap(my_cols)
    attend = call(attend_kernel, [((4, 512, 128), BF)], [], 8_000_000_000, 24, 3, "attend")
    (other,) = attend((1 - core)[None], q, k, v)
    theirs = swap(other)
    (mine,) = attend(core[None], q, k, v)
    (update,) = call(out_kernel, [((512, 1024), BF)], [], 1_000_000_000, 16, 4, "out")(
        where, mine, theirs, my_cols, their_cols
    )
    return latent[None], update[None]


def solution(mesh):
    placed = (
        P("dp", None, "space"),
        P("space", None),
        P("space", None, None),
        P(),
        P(),
        P("dp", None),
        P("dp", None),
    )
    return jax.shard_map(
        shards,
        mesh=mesh,
        in_specs=placed,
        out_specs=(P("dp", "space", None), P("dp", "space", None)),
        check_vma=False,
    )
```

```python
import math

import jax
import jax.numpy as jnp
from jax import lax
from jax.experimental import pallas as pl
from jax.experimental.layout import Layout, with_layout_constraint
from jax.experimental.pallas import tpu as pltpu
from jax.sharding import PartitionSpec as P


HEADS = 16
BF, F32 = jnp.bfloat16, jnp.float32
AXES = ("dp", "space")
def coords(dp, s):
    return dp % 4, (s // 2 % 2) * 4 + dp // 4, s // 4, s % 2


def index(x, y, z, c):
    x, y, z = x % 4, y % 8, z % 8
    return ((y % 4) * 4 + x) * 32 + z * 4 + (y // 4) * 2 + c


def send(array, move):
    pairs = [
        (dp * 32 + s, index(*move(*coords(dp, s)))) for dp in range(16) for s in range(32)
    ]
    return lax.ppermute(array, AXES, pairs)


def along(first, shift):
    def move(x, y, z, c):
        return (shift(x), y, z, c) if (c == 0) == first else (x, shift(y), z, c)

    return move


def two(place):
    return place - 2 if place % 2 else place + 2


def swap(array):
    return send(array, lambda x, y, z, c: (x, y, z, 1 - c))


def ring(array, move):
    return lax.ppermute(array, "space", [(s, move(s) % 32) for s in range(32)])


def neighbour(array):
    return ring(array, lambda s: s + 1 if s % 2 else s - 1)


def row_major(array):
    return with_layout_constraint(array, Layout(major_to_minor=(0, 1)))


def call(kernel, outs, scratch, flops, limit, n_in, name, aliases={}, n_smem=1):
    return pl.pallas_call(
        kernel,
        out_shape=[jax.ShapeDtypeStruct(s, d) for s, d in outs],
        in_specs=[pl.BlockSpec(memory_space=pltpu.SMEM)] * n_smem
        + [pl.BlockSpec(memory_space=pltpu.VMEM)] * n_in,
        out_specs=[pl.BlockSpec(memory_space=pltpu.VMEM)] * len(outs),
        scratch_shapes=[pltpu.VMEM(s, d) for s, d in scratch],
        compiler_params=pltpu.CompilerParams(vmem_limit_bytes=limit << 20),
        cost_estimate=pl.CostEstimate(flops=flops, bytes_accessed=1 << 20, transcendentals=0),
        input_output_aliases=aliases,
        name=name,
    )


def rows_at(start, count=256):
    return pl.ds(pl.multiple_of(start, 256), count)


def dot(a, b):
    return jnp.dot(a, b, preferred_element_type=F32)


def turn(cells, start, table, tall):
    count = cells.shape[1]
    tall[:100, :count] = cells[...].astype(F32)
    for j in range(0, count, 128):
        table[pl.ds(pl.multiple_of(start + j, 128), 128), :] = tall[:, j : j + 128].T


def table_kernel(where, cells, table, tall):
    tall[96:, :] = jnp.zeros((32, 1024), F32)

    def part(i, carry):
        at = pl.multiple_of(i * 1024, 1024)
        turn(cells.at[:, pl.ds(at, 1024)], at + 1024, table, tall)
        return carry

    lax.fori_loop(0, 4, part, 0)


def encode_blocks(start, index, weight, table, out, picked):
    live = lax.broadcasted_iota(jnp.int32, (16, 128), 1) < 100

    def pair(i, carry):
        for half in range(2):
            local = i * 2 + half
            b = start + local
            for j in range(128):
                picked[half, j : j + 1, :] = table[pl.ds(index[b, j], 1), :]
            summed = dot(weight[b], picked[half].astype(BF))
            rows = pl.ds(pl.multiple_of(local * 16, 16), 16)
            out[rows, :] = jnp.where(live, summed, 0.0).astype(BF)
        return carry

    lax.fori_loop(0, 8, pair, 0)


def encode_edge_kernel(where, index, weight, near, mate, filled, out, table, tall, picked):
    core = where[0]
    tall[96:, :] = jnp.zeros((32, 1024), F32)
    turn(near, core * 5120, table, tall)
    turn(mate, 5120 - core * 5120, table, tall)
    encode_blocks(core * 16, index, weight, table, out, picked)


def encode_inner_kernel(where, index, weight, table, out, picked):
    encode_blocks(16 - where[0] * 16, index, weight, table, out, picked)


def normalised(encoded, w_in, gain):
    embedded = dot(encoded, w_in)
    average = jnp.mean(embedded, axis=1, keepdims=True)
    centered = embedded - average
    spread = jnp.mean(centered * centered, axis=1, keepdims=True)
    return embedded, (centered * lax.rsqrt(spread + 1e-05) * gain).astype(BF)


def widen(w_in, wide):
    wide[96:, :] = jnp.zeros((32, 1024), BF)
    wide[:100, :] = w_in[...]


def embed_own_kernel(where, edge, inner, w_in, gain, normed, latent, wide):
    widen(w_in, wide)
    at = where[0] * 256
    for piece, start in ((edge, at), (inner, 256 - at)):
        embedded, unit = normalised(piece[...], wide[...], gain[...])
        normed[rows_at(start), :] = unit
        latent[rows_at(start), :] = embedded.astype(BF)


def embed_rest_kernel(where, near, mate, w_in, gain, normed, wide):
    widen(w_in, wide)
    at = where[0] * 256
    for piece, start in ((mate[:256], 256 - at), (mate[256:512], at), (mate[512:], 512), (near[...], 768)):
        _, unit = normalised(piece, wide[...], gain[...])
        normed[rows_at(start), :] = unit


def head_ones():
    same = lax.broadcasted_iota(jnp.int32, (256, 256), 0) // 64 == (
        lax.broadcasted_iota(jnp.int32, (256, 256), 1) // 64
    )
    return jnp.where(same, 1.0, 0.0).astype(BF)


def unit_heads(rows, ones, ref, at):
    for h in range(2):
        part = rows[:, h * 256 : (h + 1) * 256]
        squares = dot((part * part).astype(BF), ones)
        unit = (part * lax.rsqrt(squares * (1.0 / 64) + 1e-06)).astype(BF)
        ref[2 * h, at, :] = unit[:, :128]
        ref[2 * h + 1, at, :] = unit[:, 128:]


def keys_values(rows, weights, ones, k, v, at):
    unit_heads(dot(rows, weights[:, 512:1024]), ones, k, at)
    values = dot(rows, weights[:, 1024:1536]).astype(BF)
    for p in range(4):
        v[p, at, :] = values[:, p * 128 : (p + 1) * 128]


def project_tile(rows, weights, ones, q, k, v, q_at, k_at):
    unit_heads(dot(rows, weights[:, 512:1024]), ones, k, k_at)
    values = dot(rows, weights[:, 1024:1536]).astype(BF)
    for p in range(4):
        v[p, k_at, :] = values[:, p * 128 : (p + 1) * 128]
    if q_at is not None:
        unit_heads(dot(rows, weights[:, :512]), ones, q, q_at)


def project_own_kernel(where, normed, own, before, after, across, q, k, v, out_cols, weights):
    core, x, y = where[0], where[1], where[2]
    first, second = jnp.where(core == 0, x, y), jnp.where(core == 0, y, x)
    for step, piece in ((0, own), (3, before), (1, after), (2, across)):
        other = lax.rem(second + step, 4)
        for m in range(4):
            mine = first ^ m
            block = jnp.where(core == 0, other * 4 + mine, mine * 4 + other)
            rows = pl.ds(pl.multiple_of(block * 64, 64), 64)
            weights[rows, :] = piece[m * 64 : (m + 1) * 64, :1536]
            out_cols[rows, :] = piece[m * 64 : (m + 1) * 64, 1536:]
    ones = head_ones()
    start = core * 512
    for i in range(0, 512, 256):
        rows = normed[i : i + 256, :]
        project_tile(rows, weights, ones, q, k, v, rows_at(start + i), rows_at(start + i + 256))


def project_rest_kernel(where, normed, weights, q_in, k_in, v_in, q, k, v):
    core = where[0]
    ones = head_ones()
    start = 512 - core * 512
    for i in range(0, 512, 256):
        rows = normed[i : i + 256, :]
        project_tile(rows, weights, ones, q, k, v, rows_at(start + i), rows_at(start + i + 256))
    for i, at in ((512, 1280 - core * 1280), (768, core * 1280)):
        project_tile(normed[i : i + 256, :], weights, ones, q, k, v, None, rows_at(at))


def attend_kernel(shard, q, k, v, out):
    scale = math.log2(math.e) / 8.0
    low = lax.broadcasted_iota(jnp.int32, (256, 128), 1) < 64

    def tile(i, carry):
        p, part = lax.div(i, 2), lax.rem(i, 2)
        start = pl.multiple_of(shard[0] * 512, 512)
        query = q[p, pl.ds(pl.multiple_of(start + part * 256, 256), 256), :]
        keys = k[p, pl.ds(start, 1024), :]
        values = v[p, pl.ds(start, 1024), :]
        wide = jnp.concatenate([values, jnp.ones((1024, 128), BF)], axis=1)
        zero = jnp.zeros_like(query)
        mixed = []
        for head in (jnp.where(low, query, zero), jnp.where(low, zero, query)):
            scores = lax.dot_general(
                head, keys, (((1,), (1,)), ((), ())), preferred_element_type=F32
            )
            both = dot(jnp.exp2(scores * scale).astype(BF), wide)
            mixed.append(both[:, :128] / both[:, 128:])
        out[p, pl.ds(pl.multiple_of(part * 256, 256), 256), :] = jnp.where(
            low, mixed[0], mixed[1]
        ).astype(BF)
        return carry

    lax.fori_loop(0, 8, tile, 0)


def out_kernel(where, mine, theirs, my_cols, their_cols, update):
    core = where[0]
    join = lambda ref: jnp.concatenate([ref[p] for p in range(4)], axis=1)
    here, there = join(mine), join(theirs)
    near = pl.ds(pl.multiple_of(core * 512, 512), 512)
    far = pl.ds(pl.multiple_of(512 - core * 512, 512), 512)
    for cols, at in ((my_cols, near), (their_cols, far)):
        update[:, at] = (dot(here, cols[near, :]) + dot(there, cols[far, :])).astype(BF)


def shards(fields, cell_index, interp_weight, w_in, ln_gain, w_qkv, w_out):
    dp, space = lax.axis_index("dp"), lax.axis_index("space")
    core = lax.rem(space, 2)
    slot = lax.iota(jnp.int32, 4)
    where = jnp.where(slot == 0, core, jnp.where(slot == 1, lax.rem(dp, 4), lax.div(dp, 4)))

    even = core == 0
    grid_field = fields[0]
    first, last = grid_field[:, :1024], grid_field[:, 3072:]
    near_cells = row_major(neighbour(row_major(jnp.where(even, first, last))))
    mate_cells = row_major(swap(row_major(jnp.where(even, last, first))))

    halves = [
        jnp.where(even, w[:, i : i + 512], w[:, i + 512 : i + 1024])
        for w, i in ((w_qkv, 0), (w_qkv, 1024), (w_qkv, 2048), (w_out, 0))
    ]
    block = jnp.concatenate(halves, axis=1)
    pair = jnp.concatenate([block, send(block, along(True, lambda i: i ^ 1))], axis=0)
    group = jnp.concatenate([pair, send(pair, along(True, two))], axis=0)
    from_before = send(group, along(False, lambda i: i + 1))
    from_after = send(group, along(False, lambda i: i - 1))
    from_across = send(group, along(False, two))

    grown = ((6144, 128), F32)
    tall = ((128, 1024), F32)
    (table,) = call(table_kernel, [grown], [tall], 2_000_000_000, 8, 1, "table")(
        where, grid_field
    )
    picked = ((2, 128, 128), F32)
    part = ((256, 128), BF)
    edge, table = call(
        encode_edge_kernel, [part, grown], [tall, picked], 3_000_000_000, 8, 4, "edge", {5: 1}, 2
    )(where, cell_index, interp_weight, near_cells, mate_cells, table)
    near = neighbour(edge)
    (inner,) = call(encode_inner_kernel, [part], [picked], 3_000_000_000, 8, 2, "inner", {}, 2)(
        where, cell_index, interp_weight, table
    )
    mate = swap(jnp.concatenate([edge, inner, near], axis=0))

    gain = ln_gain[None]
    wide = [((128, 1024), BF)]
    own_normed, latent = call(
        embed_own_kernel,
        [((512, 1024), BF), ((512, 1024), BF)],
        wide,
        1_500_000_000,
        12,
        4,
        "embed_own",
    )(where, edge, inner, w_in, gain)
    (rest_normed,) = call(
        embed_rest_kernel, [((1024, 1024), BF)], wide, 3_000_000_000, 12, 4, "embed_rest"
    )(where, near, mate, w_in, gain)
    shapes = [((4, 1024, 128), BF), ((4, 1536, 128), BF), ((4, 1536, 128), BF)]
    q, k, v, my_cols, weights = call(
        project_own_kernel,
        shapes + [((1024, 512), BF), ((1024, 1536), BF)],
        [],
        3_000_000_000,
        12,
        5,
        "project_own",
    )(where, own_normed, group, from_before, from_after, from_across)
    q, k, v = call(
        project_rest_kernel, shapes, [], 5_000_000_000, 12, 5, "project_rest", {3: 0, 4: 1, 5: 2}
    )(where, rest_normed, weights, q, k, v)
    their_cols = swap(my_cols)
    attend = call(attend_kernel, [((4, 512, 128), BF)], [], 8_000_000_000, 24, 3, "attend")
    (other,) = attend((1 - core)[None], q, k, v)
    theirs = swap(other)
    (mine,) = attend(core[None], q, k, v)
    (update,) = call(out_kernel, [((512, 1024), BF)], [], 1_000_000_000, 16, 4, "out")(
        where, mine, theirs, my_cols, their_cols
    )
    return latent[None], update[None]


def solution(mesh):
    placed = (
        P("dp", None, "space"),
        P("space", None),
        P("space", None, None),
        P(),
        P(),
        P("dp", None),
        P("dp", None),
    )
    return jax.shard_map(
        shards,
        mesh=mesh,
        in_specs=placed,
        out_specs=(P("dp", "space", None), P("dp", "space", None)),
        check_vma=False,
    )
```

```python
import math

import jax
import jax.numpy as jnp
from jax import lax
from jax.experimental import pallas as pl
from jax.experimental.layout import Layout, with_layout_constraint
from jax.experimental.pallas import tpu as pltpu
from jax.sharding import PartitionSpec as P


BF, F32 = jnp.bfloat16, jnp.float32
AXES = ("dp", "space")


def coords(dp, s):
    return dp % 4, (s // 2 % 2) * 4 + dp // 4, s // 4, s % 2


def index(x, y, z, c):
    x, y, z = x % 4, y % 8, z % 8
    return ((y % 4) * 4 + x) * 32 + z * 4 + (y // 4) * 2 + c


def send(array, move):
    pairs = [
        (dp * 32 + s, index(*move(*coords(dp, s)))) for dp in range(16) for s in range(32)
    ]
    return lax.ppermute(array, AXES, pairs)


def along(first, shift):
    def move(x, y, z, c):
        return (shift(x), y, z, c) if (c == 0) == first else (x, shift(y), z, c)

    return move


def two(place):
    return place - 2 if place % 2 else place + 2


STEPS = (lambda i: i + 1, lambda i: i - 1, two)
SOURCES = (0, 3, 1, 2)


def swap(array):
    return send(array, lambda x, y, z, c: (x, y, z, 1 - c))


def ring(array, move):
    return lax.ppermute(array, "space", [(s, move(s) % 32) for s in range(32)])


def neighbour(array):
    return ring(array, lambda s: s + 1 if s % 2 else s - 1)


def row_major(array):
    return with_layout_constraint(array, Layout(major_to_minor=(0, 1)))


def call(kernel, outs, scratch, flops, limit, n_in, aliases={}, n_smem=1):
    return pl.pallas_call(
        kernel,
        out_shape=[jax.ShapeDtypeStruct(s, d) for s, d in outs],
        in_specs=[pl.BlockSpec(memory_space=pltpu.SMEM)] * n_smem
        + [pl.BlockSpec(memory_space=pltpu.VMEM)] * n_in,
        out_specs=[pl.BlockSpec(memory_space=pltpu.VMEM)] * len(outs),
        scratch_shapes=[pltpu.VMEM(s, d) for s, d in scratch],
        compiler_params=pltpu.CompilerParams(vmem_limit_bytes=limit << 20),
        cost_estimate=pl.CostEstimate(flops=flops, bytes_accessed=1 << 20, transcendentals=0),
        input_output_aliases=aliases,
    )


def rows_at(start, count=256):
    return pl.ds(pl.multiple_of(start, 256), count)


def dot(a, b):
    return jnp.dot(a, b, preferred_element_type=F32)


def turn(cells, start, table, tall):
    count = cells.shape[1]
    tall[:100, :count] = cells[...].astype(F32)
    for j in range(0, count, 128):
        table[pl.ds(pl.multiple_of(start + j, 128), 128), :] = tall[:, j : j + 128].T


def table_kernel(where, cells, table, tall):
    tall[96:, :] = jnp.zeros((32, 1024), F32)

    def part(i, carry):
        at = pl.multiple_of(i * 1024, 1024)
        turn(cells.at[:, pl.ds(at, 1024)], at + 1024, table, tall)
        return carry

    lax.fori_loop(0, 4, part, 0)


def encode_blocks(start, index, weight, table, out, picked):
    live = lax.broadcasted_iota(jnp.int32, (16, 128), 1) < 100

    def pair(i, carry):
        for half in range(2):
            local = i * 2 + half
            b = start + local
            for j in range(128):
                picked[half, j : j + 1, :] = table[pl.ds(index[b, j], 1), :]
            summed = dot(weight[b], picked[half].astype(BF))
            rows = pl.ds(pl.multiple_of(local * 16, 16), 16)
            out[rows, :] = jnp.where(live, summed, 0.0).astype(BF)
        return carry

    lax.fori_loop(0, 8, pair, 0)


def encode_edge_kernel(where, index, weight, near, mate, filled, out, table, tall, picked):
    core = where[0]
    tall[96:, :] = jnp.zeros((32, 1024), F32)
    turn(near, core * 5120, table, tall)
    turn(mate, 5120 - core * 5120, table, tall)
    encode_blocks(core * 16, index, weight, table, out, picked)


def encode_inner_kernel(where, index, weight, table, out, picked):
    encode_blocks(16 - where[0] * 16, index, weight, table, out, picked)


def normalised(encoded, w_in, gain):
    embedded = dot(encoded, w_in)
    average = jnp.mean(embedded, axis=1, keepdims=True)
    centered = embedded - average
    spread = jnp.mean(centered * centered, axis=1, keepdims=True)
    return embedded, (centered * lax.rsqrt(spread + 1e-05) * gain).astype(BF)


def widen(w_in, wide):
    wide[96:, :] = jnp.zeros((32, 1024), BF)
    wide[:100, :] = w_in[...]


def embed_own_kernel(where, edge, inner, w_in, gain, normed, latent, wide):
    widen(w_in, wide)
    at = where[0] * 256
    for piece, start in ((edge, at), (inner, 256 - at)):
        embedded, unit = normalised(piece[...], wide[...], gain[...])
        normed[rows_at(start), :] = unit
        latent[rows_at(start), :] = embedded.astype(BF)


def embed_rest_kernel(where, near, mate, w_in, gain, normed, wide):
    widen(w_in, wide)
    at = where[0] * 256
    for piece, start in ((mate[:256], 256 - at), (mate[256:512], at), (mate[512:], 512), (near[...], 768)):
        _, unit = normalised(piece, wide[...], gain[...])
        normed[rows_at(start), :] = unit


def head_ones():
    same = lax.broadcasted_iota(jnp.int32, (256, 256), 0) // 64 == (
        lax.broadcasted_iota(jnp.int32, (256, 256), 1) // 64
    )
    return jnp.where(same, 1.0, 0.0).astype(BF)


def unit_heads(rows, ones, ref, at):
    for h in range(2):
        part = rows[:, h * 256 : (h + 1) * 256]
        squares = dot((part * part).astype(BF), ones)
        unit = (part * lax.rsqrt(squares * (1.0 / 64) + 1e-06)).astype(BF)
        ref[2 * h, at, :] = unit[:, :128]
        ref[2 * h + 1, at, :] = unit[:, 128:]


def project_tile(rows, weights, ones, q, k, v, q_at, k_at):
    unit_heads(dot(rows, weights[:, 512:1024]), ones, k, k_at)
    values = dot(rows, weights[:, 1024:1536]).astype(BF)
    for p in range(4):
        v[p, k_at, :] = values[:, p * 128 : (p + 1) * 128]
    if q_at is not None:
        unit_heads(dot(rows, weights[:, :512]), ones, q, q_at)


def project_own_kernel(where, normed, own, before, after, across, q, k, v, out_rows, weights):
    core, x, y = where[0], where[1], where[2]
    first, second = jnp.where(core == 0, x, y), jnp.where(core == 0, y, x)
    for step, piece in zip(SOURCES, (own, before, after, across)):
        other = lax.rem(second + step, 4)
        for m in range(4):
            mine = lax.rem(first + SOURCES[m], 4)
            block = jnp.where(core == 0, other * 4 + mine, mine * 4 + other)
            rows = pl.ds(pl.multiple_of(block * 64, 64), 64)
            weights[rows, :] = piece[m * 64 : (m + 1) * 64, :1536]
            out_rows[rows, :] = piece[m * 64 : (m + 1) * 64, 1536:]
    ones = head_ones()
    start = core * 512
    for i in range(0, 512, 256):
        rows = normed[i : i + 256, :]
        project_tile(rows, weights, ones, q, k, v, rows_at(start + i), rows_at(start + i + 256))


def project_rest_kernel(where, normed, weights, q_in, k_in, v_in, q, k, v):
    core = where[0]
    ones = head_ones()
    start = 512 - core * 512
    for i in range(0, 512, 256):
        rows = normed[i : i + 256, :]
        project_tile(rows, weights, ones, q, k, v, rows_at(start + i), rows_at(start + i + 256))
    for i, at in ((512, 1280 - core * 1280), (768, core * 1280)):
        project_tile(normed[i : i + 256, :], weights, ones, q, k, v, None, rows_at(at))


def attend_kernel(shard, q, k, v, out):
    scale = math.log2(math.e) / 8.0
    low = lax.broadcasted_iota(jnp.int32, (512, 128), 1) < 64
    start = pl.multiple_of(shard[0] * 512, 512)

    def tile(p, carry):
        query = q[p, pl.ds(start, 512), :]
        zero = jnp.zeros_like(query)
        heads = (jnp.where(low, query, zero), jnp.where(low, zero, query))
        both = [None, None]
        for at in range(0, 1024, 256):
            keys = k[p, pl.ds(start + at, 256), :]
            wide = jnp.concatenate(
                [v[p, pl.ds(start + at, 256), :], jnp.ones((256, 128), BF)], axis=1
            )
            for h, head in enumerate(heads):
                scores = lax.dot_general(
                    head, keys, (((1,), (1,)), ((), ())), preferred_element_type=F32
                )
                part = dot(jnp.exp2(scores * scale).astype(BF), wide)
                both[h] = part if at == 0 else both[h] + part
        mixed = [b[:, :128] / b[:, 128:] for b in both]
        out[p, :, :] = jnp.where(low, mixed[0], mixed[1]).astype(BF)
        return carry

    lax.fori_loop(0, 4, tile, 0)


def out_kernel(where, mine, theirs, rows, update):
    core = where[0]
    join = lambda ref: jnp.concatenate([ref[p] for p in range(4)], axis=1)
    near = rows[pl.ds(pl.multiple_of(core * 512, 512), 512), :]
    far = rows[pl.ds(pl.multiple_of(512 - core * 512, 512), 512), :]
    update[...] = (dot(join(mine), near) + dot(join(theirs), far)).astype(BF)


def shards(fields, cell_index, interp_weight, w_in, ln_gain, w_qkv, w_out):
    dp, space = lax.axis_index("dp"), lax.axis_index("space")
    core = lax.rem(space, 2)
    slot = lax.iota(jnp.int32, 4)
    where = jnp.where(slot == 0, core, jnp.where(slot == 1, lax.rem(dp, 4), lax.div(dp, 4)))

    even = core == 0
    grid_field = fields[0]
    first, last = grid_field[:, :1024], grid_field[:, 3072:]
    near_cells = row_major(neighbour(row_major(jnp.where(even, first, last))))
    mate_cells = row_major(swap(row_major(jnp.where(even, last, first))))

    halves = [
        jnp.where(even, w[:, i : i + 512], w[:, i + 512 : i + 1024])
        for w, i in ((w_qkv, 0), (w_qkv, 1024), (w_qkv, 2048))
    ]
    block = jnp.concatenate(halves + [w_out], axis=1)
    line = [block]
    for shift in STEPS:
        line.append(send(block, along(True, shift)))
    group = jnp.concatenate(line, axis=0)
    gathered = [group]
    for shift in STEPS:
        gathered.append(send(group, along(False, shift)))

    grown = ((6144, 128), F32)
    tall = ((128, 1024), F32)
    (table,) = call(table_kernel, [grown], [tall], 2_000_000_000, 8, 1)(
        where, grid_field
    )
    picked = ((2, 128, 128), F32)
    part = ((256, 128), BF)
    edge, table = call(
        encode_edge_kernel, [part, grown], [tall, picked], 3_000_000_000, 8, 4, {5: 1}, 2
    )(where, cell_index, interp_weight, near_cells, mate_cells, table)
    near = neighbour(edge)
    (inner,) = call(encode_inner_kernel, [part], [picked], 3_000_000_000, 8, 2, {}, 2)(
        where, cell_index, interp_weight, table
    )
    mate = swap(jnp.concatenate([edge, inner, near], axis=0))

    gain = ln_gain[None]
    wide = [((128, 1024), BF)]
    own_normed, latent = call(
        embed_own_kernel, [((512, 1024), BF), ((512, 1024), BF)], wide, 1_500_000_000, 12, 4
    )(where, edge, inner, w_in, gain)
    (rest_normed,) = call(
        embed_rest_kernel, [((1024, 1024), BF)], wide, 3_000_000_000, 12, 4
    )(where, near, mate, w_in, gain)
    shapes = [((4, 1024, 128), BF), ((4, 1536, 128), BF), ((4, 1536, 128), BF)]
    q, k, v, out_rows, weights = call(
        project_own_kernel,
        shapes + [((1024, 1024), BF), ((1024, 1536), BF)],
        [],
        3_000_000_000,
        12,
        5,
    )(where, own_normed, *gathered)
    q, k, v = call(
        project_rest_kernel, shapes, [], 5_000_000_000, 12, 5, {3: 0, 4: 1, 5: 2}
    )(where, rest_normed, weights, q, k, v)
    attend = call(attend_kernel, [((4, 512, 128), BF)], [], 8_000_000_000, 16, 3)
    (other,) = attend((1 - core)[None], q, k, v)
    theirs = swap(other)
    (mine,) = attend(core[None], q, k, v)
    (update,) = call(out_kernel, [((512, 1024), BF)], [], 1_000_000_000, 8, 3)(
        where, mine, theirs, out_rows
    )
    return latent[None], update[None]


def solution(mesh):
    placed = (
        P("dp", None, "space"),
        P("space", None),
        P("space", None, None),
        P(),
        P(),
        P("dp", None),
        P("dp", None),
    )
    return jax.shard_map(
        shards,
        mesh=mesh,
        in_specs=placed,
        out_specs=(P("dp", "space", None), P("dp", "space", None)),
        check_vma=False,
    )
```

```python
import math

import jax
import jax.numpy as jnp
from jax import lax
from jax.experimental import pallas as pl
from jax.experimental.layout import Layout, with_layout_constraint
from jax.experimental.pallas import tpu as pltpu
from jax.sharding import PartitionSpec as P


BF, F32 = jnp.bfloat16, jnp.float32
AXES = ("dp", "space")


def coords(dp, s):
    return dp % 4, (s // 2 % 2) * 4 + dp // 4, s // 4, s % 2


def index(x, y, z, c):
    x, y, z = x % 4, y % 8, z % 8
    return ((y % 4) * 4 + x) * 32 + z * 4 + (y // 4) * 2 + c


def send(array, move):
    pairs = [
        (dp * 32 + s, index(*move(*coords(dp, s)))) for dp in range(16) for s in range(32)
    ]
    return lax.ppermute(array, AXES, pairs)


def along(first, shift):
    def move(x, y, z, c):
        return (shift(x), y, z, c) if (c == 0) == first else (x, shift(y), z, c)

    return move


def two(place):
    return place - 2 if place % 2 else place + 2


STEPS = (lambda i: i + 1, lambda i: i - 1, two)
SOURCES = (0, 3, 1, 2)


def swap(array):
    return send(array, lambda x, y, z, c: (x, y, z, 1 - c))


def ring(array, move):
    return lax.ppermute(array, "space", [(s, move(s) % 32) for s in range(32)])


def neighbour(array):
    return ring(array, lambda s: s + 1 if s % 2 else s - 1)


def row_major(array):
    return with_layout_constraint(array, Layout(major_to_minor=(0, 1)))


def call(kernel, outs, scratch, flops, limit, n_in, aliases={}, n_smem=1):
    return pl.pallas_call(
        kernel,
        out_shape=[jax.ShapeDtypeStruct(s, d) for s, d in outs],
        in_specs=[pl.BlockSpec(memory_space=pltpu.SMEM)] * n_smem
        + [pl.BlockSpec(memory_space=pltpu.VMEM)] * n_in,
        out_specs=[pl.BlockSpec(memory_space=pltpu.VMEM)] * len(outs),
        scratch_shapes=[pltpu.VMEM(s, d) for s, d in scratch],
        compiler_params=pltpu.CompilerParams(vmem_limit_bytes=limit << 20),
        cost_estimate=pl.CostEstimate(flops=flops, bytes_accessed=1 << 20, transcendentals=0),
        input_output_aliases=aliases,
    )


def rows_at(start, count=256):
    return pl.ds(pl.multiple_of(start, 256), count)


def dot(a, b):
    return jnp.dot(a, b, preferred_element_type=F32)


def turn(cells, start, table, tall):
    count = cells.shape[1]
    tall[:100, :count] = cells[...].astype(F32)
    for j in range(0, count, 128):
        table[pl.ds(pl.multiple_of(start + j, 128), 128), :] = tall[:, j : j + 128].T


def table_kernel(where, cells, table, tall):
    tall[96:, :] = jnp.zeros((32, 1024), F32)

    def part(i, carry):
        at = pl.multiple_of(i * 1024, 1024)
        turn(cells.at[:, pl.ds(at, 1024)], at + 1024, table, tall)
        return carry

    lax.fori_loop(0, 4, part, 0)


def encode_blocks(start, index, weight, table, out, picked):
    live = lax.broadcasted_iota(jnp.int32, (16, 128), 1) < 100

    def pair(i, carry):
        for half in range(2):
            local = i * 2 + half
            b = start + local
            for j in range(128):
                picked[half, j : j + 1, :] = table[pl.ds(index[b, j], 1), :]
            summed = dot(weight[b], picked[half].astype(BF))
            rows = pl.ds(pl.multiple_of(local * 16, 16), 16)
            out[rows, :] = jnp.where(live, summed, 0.0).astype(BF)
        return carry

    lax.fori_loop(0, 8, pair, 0)


def encode_edge_kernel(where, index, weight, near, mate, filled, out, table, tall, picked):
    core = where[0]
    tall[96:, :] = jnp.zeros((32, 1024), F32)
    turn(near, core * 5120, table, tall)
    turn(mate, 5120 - core * 5120, table, tall)
    encode_blocks(core * 16, index, weight, table, out, picked)


def encode_inner_kernel(where, index, weight, table, out, picked):
    encode_blocks(16 - where[0] * 16, index, weight, table, out, picked)


def normalised(encoded, w_in, gain):
    embedded = dot(encoded, w_in)
    average = jnp.mean(embedded, axis=1, keepdims=True)
    centered = embedded - average
    spread = jnp.mean(centered * centered, axis=1, keepdims=True)
    return embedded, (centered * lax.rsqrt(spread + 1e-05) * gain).astype(BF)


def widen(w_in, wide):
    wide[96:, :] = jnp.zeros((32, 1024), BF)
    wide[:100, :] = w_in[...]


def embed_own_kernel(where, edge, inner, w_in, gain, normed, latent, wide):
    widen(w_in, wide)
    at = where[0] * 256
    for piece, start in ((edge, at), (inner, 256 - at)):
        embedded, unit = normalised(piece[...], wide[...], gain[...])
        normed[rows_at(start), :] = unit
        latent[rows_at(start), :] = embedded.astype(BF)


def embed_rest_kernel(where, near, mate, w_in, gain, normed, wide):
    widen(w_in, wide)
    at = where[0] * 256
    for piece, start in ((mate[:256], 256 - at), (mate[256:512], at), (mate[512:], 512), (near[...], 768)):
        _, unit = normalised(piece, wide[...], gain[...])
        normed[rows_at(start), :] = unit


def head_ones():
    same = lax.broadcasted_iota(jnp.int32, (256, 256), 0) // 64 == (
        lax.broadcasted_iota(jnp.int32, (256, 256), 1) // 64
    )
    return jnp.where(same, 1.0, 0.0).astype(BF)


def unit_heads(rows, ones, ref, at):
    for h in range(2):
        part = rows[:, h * 256 : (h + 1) * 256]
        squares = dot((part * part).astype(BF), ones)
        unit = (part * lax.rsqrt(squares * (1.0 / 64) + 1e-06)).astype(BF)
        ref[2 * h, at, :] = unit[:, :128]
        ref[2 * h + 1, at, :] = unit[:, 128:]


def project_tile(rows, weights, ones, q, k, v, q_at, k_at):
    unit_heads(dot(rows, weights[:, 512:1024]), ones, k, k_at)
    values = dot(rows, weights[:, 1024:1536]).astype(BF)
    for p in range(4):
        v[p, k_at, :] = values[:, p * 128 : (p + 1) * 128]
    if q_at is not None:
        unit_heads(dot(rows, weights[:, :512]), ones, q, q_at)


def place(where, step, piece, weights, out_cols):
    core, x, y = where[0], where[1], where[2]
    first, second = jnp.where(core == 0, x, y), jnp.where(core == 0, y, x)
    other = lax.rem(second + step, 4)
    for m in range(4):
        mine = lax.rem(first + SOURCES[m], 4)
        block = jnp.where(core == 0, other * 4 + mine, mine * 4 + other)
        rows = pl.ds(pl.multiple_of(block * 64, 64), 64)
        weights[rows, :] = piece[m * 64 : (m + 1) * 64, :1536]
        out_cols[rows, :] = piece[m * 64 : (m + 1) * 64, 1536:]


def assemble_kernel(where, own, before, after, weights, out_cols):
    for step, piece in zip(SOURCES, (own, before, after)):
        place(where, step, piece, weights, out_cols)


def project_kernel(
    where, own, rest, across, most, most_cols, q, k, v, weights, out_cols
):
    core = where[0]
    place(where, SOURCES[3], across, weights, out_cols)
    ones = head_ones()
    for rows, start in ((own, core * 512), (rest, 512 - core * 512)):
        for i in range(0, 512, 256):
            at = rows_at(start + i), rows_at(start + i + 256)
            project_tile(rows[i : i + 256, :], weights, ones, q, k, v, *at)
    for i, at in ((512, 1280 - core * 1280), (768, core * 1280)):
        project_tile(rest[i : i + 256, :], weights, ones, q, k, v, None, rows_at(at))


def attend_kernel(shard, q, k, v, out):
    scale = math.log2(math.e) / 8.0
    low = lax.broadcasted_iota(jnp.int32, (512, 128), 1) < 64
    start = pl.multiple_of(shard[0] * 512, 512)

    def tile(p, carry):
        query = q[p, pl.ds(start, 512), :]
        zero = jnp.zeros_like(query)
        heads = (jnp.where(low, query, zero), jnp.where(low, zero, query))
        both = [None, None]
        for at in range(0, 1024, 256):
            keys = k[p, pl.ds(start + at, 256), :]
            wide = jnp.concatenate(
                [v[p, pl.ds(start + at, 256), :], jnp.ones((256, 128), BF)], axis=1
            )
            for h, head in enumerate(heads):
                scores = lax.dot_general(
                    head, keys, (((1,), (1,)), ((), ())), preferred_element_type=F32
                )
                part = dot(jnp.exp2(scores * scale).astype(BF), wide)
                both[h] = part if at == 0 else both[h] + part
        mixed = [b[:, :128] / b[:, 128:] for b in both]
        out[p, :, :] = jnp.where(low, mixed[0], mixed[1]).astype(BF)
        return carry

    lax.fori_loop(0, 4, tile, 0)


def out_kernel(where, mine, theirs, my_cols, their_cols, update):
    core = where[0]
    join = lambda ref: jnp.concatenate([ref[p] for p in range(4)], axis=1)
    here, there = join(mine), join(theirs)
    near = pl.ds(pl.multiple_of(core * 512, 512), 512)
    far = pl.ds(pl.multiple_of(512 - core * 512, 512), 512)
    for cols, at in ((my_cols, near), (their_cols, far)):
        update[:, at] = (dot(here, cols[near, :]) + dot(there, cols[far, :])).astype(BF)


def shards(fields, cell_index, interp_weight, w_in, ln_gain, w_qkv, w_out):
    dp, space = lax.axis_index("dp"), lax.axis_index("space")
    core = lax.rem(space, 2)
    slot = lax.iota(jnp.int32, 4)
    where = jnp.where(slot == 0, core, jnp.where(slot == 1, lax.rem(dp, 4), lax.div(dp, 4)))

    even = core == 0
    grid_field = fields[0]
    first, last = grid_field[:, :1024], grid_field[:, 3072:]
    near_cells = row_major(neighbour(row_major(jnp.where(even, first, last))))
    mate_cells = row_major(swap(row_major(jnp.where(even, last, first))))

    halves = [
        jnp.where(even, w[:, i : i + 512], w[:, i + 512 : i + 1024])
        for w, i in ((w_qkv, 0), (w_qkv, 1024), (w_qkv, 2048), (w_out, 0))
    ]
    block = jnp.concatenate(halves, axis=1)
    line = [block]
    for shift in STEPS:
        line.append(send(block, along(True, shift)))
    group = jnp.concatenate(line, axis=0)
    gathered = [group]
    for shift in STEPS:
        gathered.append(send(group, along(False, shift)))

    grown = ((6144, 128), F32)
    tall = ((128, 1024), F32)
    (table,) = call(table_kernel, [grown], [tall], 2_000_000_000, 8, 1)(
        where, grid_field
    )
    picked = ((2, 128, 128), F32)
    part = ((256, 128), BF)
    edge, table = call(
        encode_edge_kernel, [part, grown], [tall, picked], 3_000_000_000, 8, 4, {5: 1}, 2
    )(where, cell_index, interp_weight, near_cells, mate_cells, table)
    near = neighbour(edge)
    (inner,) = call(encode_inner_kernel, [part], [picked], 3_000_000_000, 8, 2, {}, 2)(
        where, cell_index, interp_weight, table
    )
    mate = swap(jnp.concatenate([edge, inner, near], axis=0))

    gain = ln_gain[None]
    wide = [((128, 1024), BF)]
    own_normed, latent = call(
        embed_own_kernel, [((512, 1024), BF), ((512, 1024), BF)], wide, 1_500_000_000, 12, 4
    )(where, edge, inner, w_in, gain)
    (rest_normed,) = call(
        embed_rest_kernel, [((1024, 1024), BF)], wide, 3_000_000_000, 12, 4
    )(where, near, mate, w_in, gain)
    grand = [((1024, 1536), BF), ((1024, 512), BF)]
    most = call(assemble_kernel, grand, [], 500_000_000, 8, 3)(where, *gathered[:3])
    shapes = [((4, 1024, 128), BF), ((4, 1536, 128), BF), ((4, 1536, 128), BF)]
    q, k, v, _, my_cols = call(
        project_kernel, shapes + grand, [], 8_000_000_000, 12, 5, {4: 3, 5: 4}
    )(where, own_normed, rest_normed, gathered[3], *most)
    their_cols = swap(my_cols)
    attend = call(attend_kernel, [((4, 512, 128), BF)], [], 8_000_000_000, 16, 3)
    (other,) = attend((1 - core)[None], q, k, v)
    theirs = swap(other)
    (mine,) = attend(core[None], q, k, v)
    (update,) = call(out_kernel, [((512, 1024), BF)], [], 1_000_000_000, 8, 4)(
        where, mine, theirs, my_cols, their_cols
    )
    return latent[None], update[None]


def solution(mesh):
    placed = (
        P("dp", None, "space"),
        P("space", None),
        P("space", None, None),
        P(),
        P(),
        P("dp", None),
        P("dp", None),
    )
    return jax.shard_map(
        shards,
        mesh=mesh,
        in_specs=placed,
        out_specs=(P("dp", "space", None), P("dp", "space", None)),
        check_vma=False,
    )
```

```python
import functools
import math

import jax
import jax.numpy as jnp
from jax import lax
from jax.experimental import pallas as pl
from jax.experimental.pallas import tpu as pltpu
from jax.sharding import PartitionSpec as P


BF, F32 = jnp.bfloat16, jnp.float32
AXES = ("dp", "space")


def coords(dp, s):
    return dp % 4, (s // 2 % 2) * 4 + dp // 4, s // 4, s % 2


def index(x, y, z, c):
    x, y, z = x % 4, y % 8, z % 8
    return ((y % 4) * 4 + x) * 32 + z * 4 + (y // 4) * 2 + c


def send(array, move):
    pairs = [
        (dp * 32 + s, index(*move(*coords(dp, s)))) for dp in range(16) for s in range(32)
    ]
    return lax.ppermute(array, AXES, pairs)


def along(first, shift):
    def move(x, y, z, c):
        return (shift(x), y, z, c) if (c == 0) == first else (x, shift(y), z, c)

    return move


def two(place):
    return place - 2 if place % 2 else place + 2


STEPS = (lambda i: i + 1, lambda i: i - 1, two)
SOURCES = (0, 3, 1, 2)


def swap(array):
    return send(array, lambda x, y, z, c: (x, y, z, 1 - c))


def ring(array, move):
    return lax.ppermute(array, "space", [(s, move(s) % 32) for s in range(32)])


def neighbour(array):
    return ring(array, lambda s: s + 1 if s % 2 else s - 1)


def call(kernel, outs, scratch, flops, limit, n_in, n_smem=0, any_out=()):
    spaces = [pl.ANY if i in any_out else pltpu.VMEM for i in range(len(outs))]
    return pl.pallas_call(
        kernel,
        out_shape=[jax.ShapeDtypeStruct(s, d) for s, d in outs],
        in_specs=[pl.BlockSpec(memory_space=pltpu.SMEM)] * n_smem
        + [pl.BlockSpec(memory_space=pltpu.VMEM)] * n_in,
        out_specs=[pl.BlockSpec(memory_space=m) for m in spaces],
        scratch_shapes=[pltpu.VMEM(*s) if isinstance(s, tuple) else s for s in scratch],
        compiler_params=pltpu.CompilerParams(vmem_limit_bytes=limit << 20),
        cost_estimate=pl.CostEstimate(flops=flops, bytes_accessed=1 << 20, transcendentals=0),
    )


def core_index():
    return lax.rem(lax.axis_index("space"), 2)


def rows_at(start, count=256):
    return pl.ds(pl.multiple_of(start, 256), count)


def dot(a, b):
    return jnp.dot(a, b, preferred_element_type=F32)


def turn(cells, start, table, tall):
    count = cells.shape[1]
    tall[:100, :count] = cells[...].astype(F32)
    for j in range(0, count, 128):
        table[pl.ds(pl.multiple_of(start + j, 128), 128), :] = tall[:, j : j + 128].T


def ends_kernel(cells, near, mate):
    core = core_index()
    near[...] = cells[:, pl.ds(pl.multiple_of(core * 3072, 1024), 1024)]
    mate[...] = cells[:, pl.ds(pl.multiple_of(3072 - core * 3072, 1024), 1024)]


def table_kernel(cells, w_in, table, wide, tall):
    wide[96:, :] = jnp.zeros((32, 1024), BF)
    wide[:100, :] = w_in[...]
    tall[96:, :] = jnp.zeros((32, 1024), F32)

    def part(i, carry):
        at = pl.multiple_of(i * 1024, 1024)
        turn(cells.at[:, pl.ds(at, 1024)], at, table, tall)
        return carry

    lax.fori_loop(0, 4, part, 0)


def encode_blocks(start, index, weight, table, out, at, picked):
    def pair(i, carry):
        for half in range(2):
            local = i * 2 + half
            for j in range(128):
                picked[local, j : j + 1, :] = table[pl.ds(index[start + local, j], 1), :]
        return carry

    lax.fori_loop(0, 8, pair, 0)
    live = lax.broadcasted_iota(jnp.int32, (16, 128), 1) < 100
    for local in range(16):
        summed = dot(weight[start + local], picked[local].astype(BF))
        rows = slice(at + local * 16, at + local * 16 + 16)
        out[rows, :] = jnp.where(live, summed, 0.0).astype(BF)


def encode_edge_kernel(index, weight, near, mate, own, out, table, tall, picked):
    core = core_index()
    table[1024:5120, :] = own[...]
    tall[96:, :] = jnp.zeros((32, 1024), F32)
    turn(near, core * 5120, table, tall)
    turn(mate, 5120 - core * 5120, table, tall)
    encode_blocks(core * 16, index, weight, table, out, 0, picked)


def encode_inner_kernel(index, weight, table, edge, near, out, picked):
    out[:256, :] = edge[...]
    out[512:, :] = near[...]
    encode_blocks(16 - core_index() * 16, index, weight, table, out, 256, picked)


def normalised(encoded, w_in, gain):
    embedded = dot(encoded, w_in)
    average = jnp.mean(embedded, axis=1, keepdims=True)
    centered = embedded - average
    spread = jnp.mean(centered * centered, axis=1, keepdims=True)
    return embedded, (centered * lax.rsqrt(spread + 1e-05) * gain).astype(BF)


def embed_own_kernel(packed, wide, gain, normed, latent):
    at = core_index() * 256
    for row, start in ((0, at), (256, 256 - at)):
        embedded, unit = normalised(packed[row : row + 256, :], wide[...], gain[...])
        normed[rows_at(start), :] = unit
        latent[rows_at(start), :] = embedded.astype(BF)


def embed_rest_kernel(packed, mate, wide, gain, normed):
    at = core_index() * 256
    pieces = ((mate, 0, 256 - at), (mate, 256, at), (mate, 512, 512), (packed, 512, 768))
    for piece, row, start in pieces:
        _, unit = normalised(piece[row : row + 256, :], wide[...], gain[...])
        normed[rows_at(start), :] = unit


def head_ones():
    same = lax.broadcasted_iota(jnp.int32, (256, 256), 0) // 64 == (
        lax.broadcasted_iota(jnp.int32, (256, 256), 1) // 64
    )
    return jnp.where(same, 1.0, 0.0).astype(BF)


def unit_heads(rows, ones):
    parts = []
    for h in range(2):
        part = rows[:, h * 256 : (h + 1) * 256]
        squares = dot((part * part).astype(BF), ones)
        parts.append((part * lax.rsqrt(squares * (1.0 / 64) + 1e-06)).astype(BF))
    return jnp.concatenate(parts, axis=1)


def put_heads(ref, at, rows):
    for p in range(4):
        ref[p, at, :] = rows[:, p * 128 : (p + 1) * 128]


def project_kernel(
    latent, own, rest, here, before, after, across, q, k, v, out_cols, latent_out, weights, sem
):
    copy = pltpu.make_async_copy(latent, latent_out, sem)
    copy.start()
    core = core_index()
    dp = lax.axis_index("dp")
    x, y = lax.rem(dp, 4), lax.div(dp, 4)
    first, second = jnp.where(core == 0, x, y), jnp.where(core == 0, y, x)
    for step, piece in zip(SOURCES, (here, before, after, across)):
        other = lax.rem(second + step, 4)
        for m in range(4):
            mine = lax.rem(first + SOURCES[m], 4)
            block = jnp.where(core == 0, other * 4 + mine, mine * 4 + other)
            rows = slice(m * 64, m * 64 + 64)
            weights[pl.ds(pl.multiple_of(block * 64, 64), 64), :] = piece[rows, :1536]
            half = lax.div(block, 8)
            at = pl.ds(pl.multiple_of(block * 64 - half * 512, 64), 64)
            for j in range(4):
                out_cols[half * 4 + j, at, :] = piece[rows, 1536 + j * 128 : 1664 + j * 128]
    ones = head_ones()
    for rows, start in ((own, core * 512), (rest, 512 - core * 512)):
        rows = rows[:512, :]
        at = rows_at(start + 256, 512)
        put_heads(k, at, unit_heads(dot(rows, weights[:, 512:1024]), ones))
        put_heads(q, rows_at(start, 512), unit_heads(dot(rows, weights[:, :512]), ones))
        put_heads(v, at, dot(rows, weights[:, 1024:]).astype(BF))
    far, near = rows_at(1280 - core * 1280), rows_at(core * 1280)
    rows = rest[512:, :]
    for ref, part in (
        (k, unit_heads(dot(rows, weights[:, 512:1024]), ones)),
        (v, dot(rows, weights[:, 1024:]).astype(BF)),
    ):
        put_heads(ref, far, part[:256])
        put_heads(ref, near, part[256:])
    copy.wait()


def attend_kernel(other, q, k, v, *refs):
    if other:
        cols, out = refs
        out[4:, :, :] = cols[...]
    else:
        (out,) = refs
    core = core_index()
    shard = 1 - core if other else core
    scale = math.log2(math.e) / 8.0
    low = lax.broadcasted_iota(jnp.int32, (512, 128), 1) < 64
    start = pl.multiple_of(shard * 512, 512)

    def tile(p, carry):
        query = q[p, pl.ds(start, 512), :]
        zero = jnp.zeros_like(query)
        heads = (jnp.where(low, query, zero), jnp.where(low, zero, query))
        both = [None, None]
        for at in range(0, 1024, 256):
            keys = k[p, pl.ds(start + at, 256), :]
            wide = jnp.concatenate(
                [v[p, pl.ds(start + at, 256), :], jnp.ones((256, 128), BF)], axis=1
            )
            for h, head in enumerate(heads):
                scores = lax.dot_general(
                    head, keys, (((1,), (1,)), ((), ())), preferred_element_type=F32
                )
                part = dot(jnp.exp2(scores * scale).astype(BF), wide)
                both[h] = part if at == 0 else both[h] + part
        mixed = [b[:, :128] / b[:, 128:] for b in both]
        out[p, :, :] = jnp.where(low, mixed[0], mixed[1]).astype(BF)
        return carry

    lax.fori_loop(0, 4, tile, 0)


def out_kernel(mine, my_cols, theirs, update, done, sem):
    core = core_index()

    def join(ref, first, rows):
        return jnp.concatenate([ref[first + p, rows, :] for p in range(4)], axis=1)

    near = pl.ds(pl.multiple_of(core * 512, 512), 512)
    far = pl.ds(pl.multiple_of(512 - core * 512, 512), 512)
    every = slice(0, 512)
    copies = []
    for i in range(2):
        rows = slice(i * 256, i * 256 + 256)
        here, there = join(mine, 0, rows), join(theirs, 0, rows)
        for ref, skip, at in ((my_cols, 0, near), (theirs, 4, far)):
            top = join(ref, skip + core * 4, every)
            low = join(ref, skip + 4 - core * 4, every)
            done[rows, at] = (dot(here, top) + dot(there, low)).astype(BF)
        copies.append(pltpu.make_async_copy(done.at[rows], update.at[rows], sem.at[i]))
        copies[i].start()
    for copy in copies:
        copy.wait()


def shards(fields, cell_index, interp_weight, w_in, ln_gain, w_qkv, w_out):
    core = core_index()
    even = core == 0
    grid_field = fields[0]
    end = ((100, 1024), BF)
    near_cells, mate_cells = call(ends_kernel, [end, end], [], 100_000_000, 8, 1)(grid_field)
    near_cells = neighbour(near_cells)
    mate_cells = swap(mate_cells)

    halves = [
        jnp.where(even, w[:, i : i + 512], w[:, i + 512 : i + 1024])
        for w, i in ((w_qkv, 0), (w_qkv, 1024), (w_qkv, 2048), (w_out, 0))
    ]
    block = jnp.concatenate(halves, axis=1)
    line = [block]
    for shift in STEPS:
        line.append(send(block, along(True, shift)))
    group = jnp.concatenate(line, axis=0)
    gathered = [group]
    for shift in STEPS:
        gathered.append(send(group, along(False, shift)))

    grown, tall = ((6144, 128), F32), ((128, 1024), F32)
    table, wide = call(
        table_kernel, [((4096, 128), F32), ((128, 1024), BF)], [tall], 2_000_000_000, 8, 2
    )(grid_field, w_in)
    picked = ((16, 128, 128), F32)
    edge, table = call(
        encode_edge_kernel, [((256, 128), BF), grown], [tall, picked], 3_000_000_000, 8, 4, 1
    )(cell_index, interp_weight, near_cells, mate_cells, table)
    near = neighbour(edge)
    (packed,) = call(
        encode_inner_kernel, [((768, 128), BF)], [picked], 3_000_000_000, 8, 4, 1
    )(cell_index, interp_weight, table, edge, near)
    mate = swap(packed)

    gain = ln_gain[None]
    tile = ((512, 1024), BF)
    own_normed, latent = call(
        embed_own_kernel, [tile, tile], [], 1_500_000_000, 12, 3
    )(packed, wide, gain)
    (rest_normed,) = call(
        embed_rest_kernel, [((1024, 1024), BF)], [], 3_000_000_000, 12, 4
    )(packed, mate, wide, gain)
    q, k, v, my_cols, latent = call(
        project_kernel,
        [((4, n, 128), BF) for n in (1024, 1536, 1536)] + [((8, 512, 128), BF), tile],
        [((1024, 1536), BF), pltpu.SemaphoreType.DMA],
        8_000_000_000,
        16,
        7,
        any_out=(4,),
    )(latent, own_normed, rest_normed, *gathered)

    def attend(other, *args):
        kernel = functools.partial(attend_kernel, other)
        outs = [((12 if other else 4, 512, 128), BF)]
        return call(kernel, outs, [], 8_000_000_000, 16, len(args))(*args)[0]

    theirs = swap(attend(True, q, k, v, my_cols))
    mine = attend(False, q, k, v)
    (update,) = call(
        out_kernel,
        [tile],
        [tile, pltpu.SemaphoreType.DMA((2,))],
        1_000_000_000,
        12,
        3,
        any_out=(0,),
    )(mine, my_cols, theirs)
    return latent[None], update[None]


def solution(mesh):
    placed = (
        P("dp", None, "space"),
        P("space", None),
        P("space", None, None),
        P(),
        P(),
        P("dp", None),
        P("dp", None),
    )
    return jax.shard_map(
        shards,
        mesh=mesh,
        in_specs=placed,
        out_specs=(P("dp", "space", None), P("dp", "space", None)),
        check_vma=False,
    )
```

```python
import functools
import math

import jax
import jax.numpy as jnp
from jax import lax
from jax.experimental import pallas as pl
from jax.experimental.pallas import tpu as pltpu
from jax.sharding import PartitionSpec as P


BF, F32 = jnp.bfloat16, jnp.float32
AXES = ("dp", "space")


def coords(dp, s):
    return dp % 4, (s // 2 % 2) * 4 + dp // 4, s // 4, s % 2


def index(x, y, z, c):
    x, y, z = x % 4, y % 8, z % 8
    return ((y % 4) * 4 + x) * 32 + z * 4 + (y // 4) * 2 + c


def send(array, move):
    pairs = [
        (dp * 32 + s, index(*move(*coords(dp, s)))) for dp in range(16) for s in range(32)
    ]
    return lax.ppermute(array, AXES, pairs)


def along(first, shift):
    def move(x, y, z, c):
        return (shift(x), y, z, c) if (c == 0) == first else (x, shift(y), z, c)

    return move


def two(place):
    return place - 2 if place % 2 else place + 2


STEPS = (lambda i: i + 1, lambda i: i - 1, two)
SOURCES = (0, 3, 1, 2)


def swap(array):
    return send(array, lambda x, y, z, c: (x, y, z, 1 - c))


def ring(array, move):
    return lax.ppermute(array, "space", [(s, move(s) % 32) for s in range(32)])


def neighbour(array):
    return ring(array, lambda s: s + 1 if s % 2 else s - 1)


def call(kernel, outs, scratch, flops, limit, n_in, n_smem=0, any_out=(), n_hbm=0):
    spaces = [pl.ANY if i in any_out else pltpu.VMEM for i in range(len(outs))]
    return pl.pallas_call(
        kernel,
        out_shape=[jax.ShapeDtypeStruct(s, d) for s, d in outs],
        in_specs=[pl.BlockSpec(memory_space=pltpu.SMEM)] * n_smem
        + [pl.BlockSpec(memory_space=pltpu.HBM)] * n_hbm
        + [pl.BlockSpec(memory_space=pltpu.VMEM)] * n_in,
        out_specs=[pl.BlockSpec(memory_space=m) for m in spaces],
        scratch_shapes=[pltpu.VMEM(*s) if isinstance(s, tuple) else s for s in scratch],
        compiler_params=pltpu.CompilerParams(vmem_limit_bytes=limit << 20),
        cost_estimate=pl.CostEstimate(flops=flops, bytes_accessed=1 << 20, transcendentals=0),
    )


def core_index():
    return lax.rem(lax.axis_index("space"), 2)


def rows_at(start, count=256):
    return pl.ds(pl.multiple_of(start, 256), count)


def dot(a, b):
    return jnp.dot(a, b, preferred_element_type=F32)


def turn(cells, start, table, tall):
    count = cells.shape[1]
    tall[:100, :count] = cells[...].astype(F32)
    for j in range(0, count, 128):
        table[pl.ds(pl.multiple_of(start + j, 128), 128), :] = tall[:, j : j + 128].T


def front_kernel(fields, w_qkv, w_out, block, near, mate, cells, sem):
    core = core_index()

    def part(source, start, count):
        return source.at[:, pl.ds(pl.multiple_of(start, 128), count)]

    moves = [
        (part(w_qkv, i * 1024 + core * 512, 512), block.at[:, i * 512 : i * 512 + 512])
        for i in range(3)
    ]
    moves += [
        (part(w_out, core * 512, 512), block.at[:, 1536:]),
        (part(fields, core * 3072, 1024), near),
        (part(fields, 3072 - core * 3072, 1024), mate),
        (fields, cells),
    ]
    copies = [pltpu.make_async_copy(a, b, sem.at[i]) for i, (a, b) in enumerate(moves)]
    for copy in copies:
        copy.start()
    for copy in copies:
        copy.wait()


def table_kernel(cells, w_in, table, wide, tall):
    wide[96:, :] = jnp.zeros((32, 1024), BF)
    wide[:100, :] = w_in[...]
    tall[96:, :] = jnp.zeros((32, 1024), F32)

    def part(i, carry):
        at = pl.multiple_of(i * 1024, 1024)
        turn(cells.at[:, pl.ds(at, 1024)], at, table, tall)
        return carry

    lax.fori_loop(0, 4, part, 0)


def encode_blocks(start, index, weight, table, out, picked):
    def pair(i, carry):
        for half in range(2):
            local = i * 2 + half
            for j in range(128):
                picked[local, j : j + 1, :] = table[pl.ds(index[start + local, j], 1), :]
        return carry

    lax.fori_loop(0, 8, pair, 0)
    live = lax.broadcasted_iota(jnp.int32, (16, 128), 1) < 100
    for local in range(16):
        summed = dot(weight[start + local], picked[local].astype(BF))
        rows = slice(local * 16, local * 16 + 16)
        out[rows, :] = jnp.where(live, summed, 0.0).astype(BF)


def encode_edge_kernel(index, weight, near, mate, own, out, table, tall, picked):
    core = core_index()
    table[1024:5120, :] = own[...]
    tall[96:, :] = jnp.zeros((32, 1024), F32)
    turn(near, core * 5120, table, tall)
    turn(mate, 5120 - core * 5120, table, tall)
    encode_blocks(core * 16, index, weight, table, out, picked)


def encode_inner_kernel(index, weight, table, out, picked):
    encode_blocks(16 - core_index() * 16, index, weight, table, out, picked)


def normalised(encoded, w_in, gain):
    embedded = dot(encoded, w_in)
    average = jnp.mean(embedded, axis=1, keepdims=True)
    centered = embedded - average
    spread = jnp.mean(centered * centered, axis=1, keepdims=True)
    return embedded, (centered * lax.rsqrt(spread + 1e-05) * gain).astype(BF)


def embed_own_kernel(packed, wide, gain, normed, latent):
    at = core_index() * 256
    for row, start in ((0, at), (256, 256 - at)):
        embedded, unit = normalised(packed[row : row + 256, :], wide[...], gain[...])
        normed[rows_at(start), :] = unit
        latent[rows_at(start), :] = embedded.astype(BF)


def embed_rest_kernel(packed, mate, wide, gain, normed):
    at = core_index() * 256
    pieces = ((mate, 0, 256 - at), (mate, 256, at), (mate, 512, 512), (packed, 512, 768))
    for piece, row, start in pieces:
        _, unit = normalised(piece[row : row + 256, :], wide[...], gain[...])
        normed[rows_at(start), :] = unit


def head_ones():
    same = lax.broadcasted_iota(jnp.int32, (256, 256), 0) // 64 == (
        lax.broadcasted_iota(jnp.int32, (256, 256), 1) // 64
    )
    return jnp.where(same, 1.0, 0.0).astype(BF)


def unit_heads(rows, ones):
    parts = []
    for h in range(2):
        part = rows[:, h * 256 : (h + 1) * 256]
        squares = dot((part * part).astype(BF), ones)
        parts.append((part * lax.rsqrt(squares * (1.0 / 64) + 1e-06)).astype(BF))
    return jnp.concatenate(parts, axis=1)


def put_heads(ref, at, rows):
    for p in range(4):
        ref[p, at, :] = rows[:, p * 128 : (p + 1) * 128]


def project_kernel(
    latent, own, rest, here, before, after, across, q, k, v, out_cols, latent_out, weights, sem
):
    copy = pltpu.make_async_copy(latent, latent_out, sem)
    copy.start()
    core = core_index()
    dp = lax.axis_index("dp")
    x, y = lax.rem(dp, 4), lax.div(dp, 4)
    first, second = jnp.where(core == 0, x, y), jnp.where(core == 0, y, x)
    for step, piece in zip(SOURCES, (here, before, after, across)):
        other = lax.rem(second + step, 4)
        for m in range(4):
            mine = lax.rem(first + SOURCES[m], 4)
            block = jnp.where(core == 0, other * 4 + mine, mine * 4 + other)
            rows = slice(m * 64, m * 64 + 64)
            weights[pl.ds(pl.multiple_of(block * 64, 64), 64), :] = piece[rows, :1536]
            half = lax.div(block, 8)
            at = pl.ds(pl.multiple_of(block * 64 - half * 512, 64), 64)
            for j in range(4):
                out_cols[half * 4 + j, at, :] = piece[rows, 1536 + j * 128 : 1664 + j * 128]
    ones = head_ones()
    for rows, start in ((own, core * 512), (rest, 512 - core * 512)):
        rows = rows[:512, :]
        at = rows_at(start + 256, 512)
        put_heads(k, at, unit_heads(dot(rows, weights[:, 512:1024]), ones))
        put_heads(q, rows_at(start, 512), unit_heads(dot(rows, weights[:, :512]), ones))
        put_heads(v, at, dot(rows, weights[:, 1024:]).astype(BF))
    far, near = rows_at(1280 - core * 1280), rows_at(core * 1280)
    rows = rest[512:, :]
    for ref, part in (
        (k, unit_heads(dot(rows, weights[:, 512:1024]), ones)),
        (v, dot(rows, weights[:, 1024:]).astype(BF)),
    ):
        put_heads(ref, far, part[:256])
        put_heads(ref, near, part[256:])
    copy.wait()


def attend_kernel(other, q, k, v, *refs):
    if other:
        cols, out = refs
        out[4:, :, :] = cols[...]
    else:
        (out,) = refs
    core = core_index()
    shard = 1 - core if other else core
    scale = math.log2(math.e) / 8.0
    low = lax.broadcasted_iota(jnp.int32, (512, 128), 1) < 64
    start = pl.multiple_of(shard * 512, 512)

    def tile(p, carry):
        query = q[p, pl.ds(start, 512), :]
        zero = jnp.zeros_like(query)
        heads = (jnp.where(low, query, zero), jnp.where(low, zero, query))
        both = [None, None]
        for at in range(0, 1024, 256):
            keys = k[p, pl.ds(start + at, 256), :]
            wide = jnp.concatenate(
                [v[p, pl.ds(start + at, 256), :], jnp.ones((256, 128), BF)], axis=1
            )
            for h, head in enumerate(heads):
                scores = lax.dot_general(
                    head, keys, (((1,), (1,)), ((), ())), preferred_element_type=F32
                )
                part = dot(jnp.exp2(scores * scale).astype(BF), wide)
                both[h] = part if at == 0 else both[h] + part
        mixed = [b[:, :128] / b[:, 128:] for b in both]
        out[p, :, :] = jnp.where(low, mixed[0], mixed[1]).astype(BF)
        return carry

    lax.fori_loop(0, 4, tile, 0)


def out_kernel(mine, my_cols, theirs, update, done, sem):
    core = core_index()

    def join(ref, first, rows):
        return jnp.concatenate([ref[first + p, rows, :] for p in range(4)], axis=1)

    near = pl.ds(pl.multiple_of(core * 512, 512), 512)
    far = pl.ds(pl.multiple_of(512 - core * 512, 512), 512)
    every = slice(0, 512)
    copies = []
    for i in range(2):
        rows = slice(i * 256, i * 256 + 256)
        here, there = join(mine, 0, rows), join(theirs, 0, rows)
        for ref, skip, at in ((my_cols, 0, near), (theirs, 4, far)):
            top = join(ref, skip + core * 4, every)
            low = join(ref, skip + 4 - core * 4, every)
            done[rows, at] = (dot(here, top) + dot(there, low)).astype(BF)
        copies.append(pltpu.make_async_copy(done.at[rows], update.at[rows], sem.at[i]))
        copies[i].start()
    for copy in copies:
        copy.wait()


def shards(fields, cell_index, interp_weight, w_in, ln_gain, w_qkv, w_out):
    end = ((100, 1024), BF)
    block, near_cells, mate_cells, cells = call(
        front_kernel,
        [((64, 2048), BF), end, end, ((100, 4096), BF)],
        [pltpu.SemaphoreType.DMA((7,))],
        100_000_000,
        8,
        0,
        n_hbm=3,
    )(*(pltpu.with_memory_space_constraint(a, pltpu.HBM) for a in (fields[0], w_qkv, w_out)))
    near_cells = neighbour(near_cells)
    mate_cells = swap(mate_cells)

    line = [block]
    for shift in STEPS:
        line.append(send(block, along(True, shift)))
    group = jnp.concatenate(line, axis=0)
    gathered = [group]
    for shift in STEPS:
        gathered.append(send(group, along(False, shift)))

    grown, tall = ((6144, 128), F32), ((128, 1024), F32)
    table, wide = call(
        table_kernel, [((4096, 128), F32), ((128, 1024), BF)], [tall], 2_000_000_000, 8, 2
    )(cells, w_in)
    picked = ((16, 128, 128), F32)
    edge, table = call(
        encode_edge_kernel, [((256, 128), BF), grown], [tall, picked], 3_000_000_000, 8, 4, 1
    )(cell_index, interp_weight, near_cells, mate_cells, table)
    near = neighbour(edge)
    (inner,) = call(
        encode_inner_kernel, [((256, 128), BF)], [picked], 3_000_000_000, 8, 2, 1
    )(cell_index, interp_weight, table)
    packed = jnp.concatenate([edge, inner, near], axis=0)
    mate = swap(packed)

    gain = ln_gain[None]
    tile = ((512, 1024), BF)
    own_normed, latent = call(
        embed_own_kernel, [tile, tile], [], 1_500_000_000, 12, 3
    )(packed, wide, gain)
    (rest_normed,) = call(
        embed_rest_kernel, [((1024, 1024), BF)], [], 3_000_000_000, 12, 4
    )(packed, mate, wide, gain)
    q, k, v, my_cols, latent = call(
        project_kernel,
        [((4, n, 128), BF) for n in (1024, 1536, 1536)] + [((8, 512, 128), BF), tile],
        [((1024, 1536), BF), pltpu.SemaphoreType.DMA],
        8_000_000_000,
        16,
        7,
        any_out=(4,),
    )(latent, own_normed, rest_normed, *gathered)

    def attend(other, *args):
        kernel = functools.partial(attend_kernel, other)
        outs = [((12 if other else 4, 512, 128), BF)]
        return call(kernel, outs, [], 8_000_000_000, 16, len(args))(*args)[0]

    theirs = swap(attend(True, q, k, v, my_cols))
    mine = attend(False, q, k, v)
    (update,) = call(
        out_kernel,
        [tile],
        [tile, pltpu.SemaphoreType.DMA((2,))],
        1_000_000_000,
        12,
        3,
        any_out=(0,),
    )(mine, my_cols, theirs)
    return latent[None], update[None]


def solution(mesh):
    placed = (
        P("dp", None, "space"),
        P("space", None),
        P("space", None, None),
        P(),
        P(),
        P("dp", None),
        P("dp", None),
    )
    return jax.shard_map(
        shards,
        mesh=mesh,
        in_specs=placed,
        out_specs=(P("dp", "space", None), P("dp", "space", None)),
        check_vma=False,
    )
```

```python
import functools
import math

import jax
import jax.numpy as jnp
from jax import lax
from jax.experimental import pallas as pl
from jax.experimental.pallas import tpu as pltpu
from jax.sharding import PartitionSpec as P


BF, F32 = jnp.bfloat16, jnp.float32
AXES = ("dp", "space")


def coords(dp, s):
    return dp % 4, (s // 2 % 2) * 4 + dp // 4, s // 4, s % 2


def index(x, y, z, c):
    x, y, z = x % 4, y % 8, z % 8
    return ((y % 4) * 4 + x) * 32 + z * 4 + (y // 4) * 2 + c


def send(array, move):
    pairs = [
        (dp * 32 + s, index(*move(*coords(dp, s)))) for dp in range(16) for s in range(32)
    ]
    return lax.ppermute(array, AXES, pairs)


def along(first, shift):
    def move(x, y, z, c):
        return (shift(x), y, z, c) if (c == 0) == first else (x, shift(y), z, c)

    return move


def two(place):
    return place - 2 if place % 2 else place + 2


STEPS = (lambda i: i + 1, lambda i: i - 1, two)
SOURCES = (0, 3, 1, 2)


def swap(array):
    return send(array, lambda x, y, z, c: (x, y, z, 1 - c))


def ring(array, move):
    return lax.ppermute(array, "space", [(s, move(s) % 32) for s in range(32)])


def neighbour(array):
    return ring(array, lambda s: s + 1 if s % 2 else s - 1)


def call(kernel, outs, scratch, flops, limit, n_in, n_smem=0, any_out=(), n_hbm=0):
    spaces = [pl.ANY if i in any_out else pltpu.VMEM for i in range(len(outs))]
    return pl.pallas_call(
        kernel,
        out_shape=[jax.ShapeDtypeStruct(s, d) for s, d in outs],
        in_specs=[pl.BlockSpec(memory_space=pltpu.SMEM)] * n_smem
        + [pl.BlockSpec(memory_space=pltpu.HBM)] * n_hbm
        + [pl.BlockSpec(memory_space=pltpu.VMEM)] * n_in,
        out_specs=[pl.BlockSpec(memory_space=m) for m in spaces],
        scratch_shapes=[pltpu.VMEM(*s) if isinstance(s, tuple) else s for s in scratch],
        compiler_params=pltpu.CompilerParams(vmem_limit_bytes=limit << 20),
        cost_estimate=pl.CostEstimate(flops=flops, bytes_accessed=1 << 20, transcendentals=0),
    )


def core_index():
    return lax.rem(lax.axis_index("space"), 2)


def rows_at(start, count=256):
    return pl.ds(pl.multiple_of(start, 256), count)


def dot(a, b):
    return jnp.dot(a, b, preferred_element_type=F32)


def turn(cells, start, table, tall):
    count = cells.shape[1]
    tall[:100, :count] = cells[...].astype(F32)
    for j in range(0, count, 128):
        table[pl.ds(pl.multiple_of(start + j, 128), 128), :] = tall[:, j : j + 128].T


def front_kernel(fields, w_qkv, w_out, block, near, mate, cells, sem):
    core = core_index()

    def part(source, start, count):
        return source.at[:, pl.ds(pl.multiple_of(start, 128), count)]

    moves = [
        (part(w_qkv, i * 1024 + core * 512, 512), block.at[:, i * 512 : i * 512 + 512])
        for i in range(3)
    ]
    moves += [
        (part(w_out, core * 512, 512), block.at[:, 1536:]),
        (part(fields, core * 3072, 1024), near),
        (part(fields, 3072 - core * 3072, 1024), mate),
        (fields, cells),
    ]
    copies = [pltpu.make_async_copy(a, b, sem.at[i]) for i, (a, b) in enumerate(moves)]
    for copy in copies:
        copy.start()
    for copy in copies:
        copy.wait()


def sources_of(i):
    return jnp.where(i == 0, 0, jnp.where(i == 1, 3, i - 1))


def table_kernel(cells, w_in, gain, table, wide, mixed, mixed_gain, tall):
    wide[96:, :] = jnp.zeros((32, 1024), BF)
    wide[:100, :] = w_in[...]
    tall[96:, :] = jnp.zeros((32, 1024), F32)

    def part(i, carry):
        at = pl.multiple_of(i * 1024, 1024)
        turn(cells.at[:, pl.ds(at, 1024)], at, table, tall)
        return carry

    lax.fori_loop(0, 4, part, 0)

    core, dp = core_index(), lax.axis_index("dp")
    x, y = lax.rem(dp, 4), lax.div(dp, 4)
    place = lax.broadcasted_iota(jnp.int32, (256, 1024), 1)
    group, member = sources_of(place >> 8), sources_of((place >> 6) & 3)
    row = (y + jnp.where(core == 0, group, member)) & 3
    column = (x + jnp.where(core == 0, member, group)) & 3
    source = row * 256 + column * 64 + (place & 63)
    high = gain[...].astype(BF).astype(F32)
    middle = (gain[...] - high).astype(BF).astype(F32)
    low = gain[...] - high - middle
    line = lax.broadcasted_iota(jnp.int32, (16, 1024), 0)
    parts = jnp.where(line == 0, high, jnp.where(line == 1, middle, jnp.where(line == 2, low, 0.0)))
    parts = parts.astype(BF)
    total, total_gain = None, None
    for i in range(0, 1024, 256):
        here = lax.broadcasted_iota(jnp.int32, (256, 1024), 0) + i
        move = jnp.where(here == source, 1.0, 0.0).astype(BF)
        one, two_ = dot(wide[:, i : i + 256], move), dot(parts[:, i : i + 256], move)
        total = one if i == 0 else total + one
        total_gain = two_ if i == 0 else total_gain + two_
    mixed[...] = total.astype(BF)
    mixed_gain[...] = jnp.sum(total_gain, axis=0, keepdims=True)


def encode_blocks(start, index, weight, table, out, picked):
    def pair(i, carry):
        for half in range(2):
            local = i * 2 + half
            for j in range(128):
                picked[local, j : j + 1, :] = table[pl.ds(index[start + local, j], 1), :]
        return carry

    lax.fori_loop(0, 8, pair, 0)
    live = lax.broadcasted_iota(jnp.int32, (16, 128), 1) < 100
    for local in range(16):
        summed = dot(weight[start + local], picked[local].astype(BF))
        rows = slice(local * 16, local * 16 + 16)
        out[rows, :] = jnp.where(live, summed, 0.0).astype(BF)


def encode_edge_kernel(index, weight, near, mate, own, out, table, tall, picked):
    core = core_index()
    table[1024:5120, :] = own[...]
    tall[96:, :] = jnp.zeros((32, 1024), F32)
    turn(near, core * 5120, table, tall)
    turn(mate, 5120 - core * 5120, table, tall)
    encode_blocks(core * 16, index, weight, table, out, picked)


def encode_inner_kernel(index, weight, table, out, picked):
    encode_blocks(16 - core_index() * 16, index, weight, table, out, picked)


def normalised(encoded, w_in, gain):
    embedded = dot(encoded, w_in)
    average = jnp.mean(embedded, axis=1, keepdims=True)
    centered = embedded - average
    spread = jnp.mean(centered * centered, axis=1, keepdims=True)
    return (centered * lax.rsqrt(spread + 1e-05) * gain).astype(BF)


def embed_own_kernel(packed, wide, mixed, gain, normed, latent):
    at = core_index() * 256
    for row, start in ((0, at), (256, 256 - at)):
        piece = packed[row : row + 256, :]
        normed[rows_at(start), :] = normalised(piece, mixed[...], gain[...])
        latent[rows_at(start), :] = dot(piece, wide[...]).astype(BF)


def embed_rest_kernel(packed, mate, mixed, gain, normed):
    at = core_index() * 256
    pieces = ((mate, 0, 256 - at), (mate, 256, at), (mate, 512, 512), (packed, 512, 768))
    for piece, row, start in pieces:
        normed[rows_at(start), :] = normalised(piece[row : row + 256, :], mixed[...], gain[...])


def head_ones():
    same = lax.broadcasted_iota(jnp.int32, (256, 256), 0) // 64 == (
        lax.broadcasted_iota(jnp.int32, (256, 256), 1) // 64
    )
    return jnp.where(same, 1.0, 0.0).astype(BF)


def unit_heads(rows, ones):
    parts = []
    for h in range(2):
        part = rows[:, h * 256 : (h + 1) * 256]
        squares = dot((part * part).astype(BF), ones)
        parts.append((part * lax.rsqrt(squares * (1.0 / 64) + 1e-06)).astype(BF))
    return jnp.concatenate(parts, axis=1)


def put_heads(ref, at, rows):
    for p in range(4):
        ref[p, at, :] = rows[:, p * 128 : (p + 1) * 128]


def first_kernel(latent, own, rest, here, before, after, mine, mates, sides, latent_out, sem):
    copy = pltpu.make_async_copy(latent, latent_out, sem)
    copy.start()
    for rows, sums, skip in ((own[...], mine, 0), (rest[:512, :], mates, 0), (rest[512:, :], sides, 512)):
        for col in range(skip, 1536, 512):
            cols = slice(col, col + 512)
            weights = jnp.concatenate([here[:, cols], before[:, cols], after[:, cols]], axis=0)
            sums[:, col - skip : col - skip + 512] = dot(rows[:, :768], weights)
    copy.wait()


def project_kernel(own, rest, across, mine, mates, sides, q, k, v):
    core = core_index()
    ones = head_ones()

    def whole(rows, sums, skip, col):
        return sums[:, col - skip : col - skip + 512] + dot(rows, across[:, col : col + 512])

    for rows, sums, start in (
        (own[:, 768:], mine, core * 512),
        (rest[:512, 768:], mates, 512 - core * 512),
    ):
        at = rows_at(start + 256, 512)
        put_heads(k, at, unit_heads(whole(rows, sums, 0, 512), ones))
        put_heads(q, rows_at(start, 512), unit_heads(whole(rows, sums, 0, 0), ones))
        put_heads(v, at, whole(rows, sums, 0, 1024).astype(BF))
    far, near = rows_at(1280 - core * 1280), rows_at(core * 1280)
    rows = rest[512:, 768:]
    for ref, part in (
        (k, unit_heads(whole(rows, sides, 512, 512), ones)),
        (v, whole(rows, sides, 512, 1024).astype(BF)),
    ):
        put_heads(ref, far, part[:256])
        put_heads(ref, near, part[256:])


def place_columns(pieces, out):
    core, dp = core_index(), lax.axis_index("dp")
    x, y = lax.rem(dp, 4), lax.div(dp, 4)
    first, second = jnp.where(core == 0, x, y), jnp.where(core == 0, y, x)
    for step, piece in zip(SOURCES, pieces):
        other = lax.rem(second + step, 4)
        for m in range(4):
            mine = lax.rem(first + SOURCES[m], 4)
            block = jnp.where(core == 0, other * 4 + mine, mine * 4 + other)
            half = lax.div(block, 8)
            at = pl.ds(pl.multiple_of(block * 64 - half * 512, 64), 64)
            for j in range(4):
                cols = slice(1536 + j * 128, 1664 + j * 128)
                out[4 + half * 4 + j, at, :] = piece[m * 64 : m * 64 + 64, cols]


def attend_kernel(other, q, k, v, *refs):
    *pieces, out = refs
    if other:
        place_columns(pieces, out)
    core = core_index()
    shard = 1 - core if other else core
    scale = math.log2(math.e) / 8.0
    low = lax.broadcasted_iota(jnp.int32, (512, 128), 1) < 64
    start = pl.multiple_of(shard * 512, 512)

    def tile(p, carry):
        query = q[p, pl.ds(start, 512), :]
        zero = jnp.zeros_like(query)
        heads = (jnp.where(low, query, zero), jnp.where(low, zero, query))
        both = [None, None]
        for at in range(0, 1024, 256):
            keys = k[p, pl.ds(start + at, 256), :]
            wide = jnp.concatenate(
                [v[p, pl.ds(start + at, 256), :], jnp.ones((256, 128), BF)], axis=1
            )
            for h, head in enumerate(heads):
                scores = lax.dot_general(
                    head, keys, (((1,), (1,)), ((), ())), preferred_element_type=F32
                )
                part = dot(jnp.exp2(scores * scale).astype(BF), wide)
                both[h] = part if at == 0 else both[h] + part
        mixed = [b[:, :128] / b[:, 128:] for b in both]
        out[p, :, :] = jnp.where(low, mixed[0], mixed[1]).astype(BF)
        return carry

    lax.fori_loop(0, 4, tile, 0)


def out_kernel(mine, sent, theirs, update, done, sem):
    core = core_index()

    def join(ref, first, rows):
        return jnp.concatenate([ref[first + p, rows, :] for p in range(4)], axis=1)

    near = pl.ds(pl.multiple_of(core * 512, 512), 512)
    far = pl.ds(pl.multiple_of(512 - core * 512, 512), 512)
    every = slice(0, 512)
    copies = []
    for i in range(2):
        rows = slice(i * 256, i * 256 + 256)
        here, there = join(mine, 0, rows), join(theirs, 0, rows)
        for ref, at in ((sent, near), (theirs, far)):
            top = join(ref, 4 + core * 4, every)
            low = join(ref, 8 - core * 4, every)
            done[rows, at] = (dot(here, top) + dot(there, low)).astype(BF)
        copies.append(pltpu.make_async_copy(done.at[rows], update.at[rows], sem.at[i]))
        copies[i].start()
    for copy in copies:
        copy.wait()


def shards(fields, cell_index, interp_weight, w_in, ln_gain, w_qkv, w_out):
    end = ((100, 1024), BF)
    block, near_cells, mate_cells, cells = call(
        front_kernel,
        [((64, 2048), BF), end, end, ((100, 4096), BF)],
        [pltpu.SemaphoreType.DMA((7,))],
        100_000_000,
        8,
        0,
        n_hbm=3,
    )(*(pltpu.with_memory_space_constraint(a, pltpu.HBM) for a in (fields[0], w_qkv, w_out)))
    near_cells = neighbour(near_cells)
    mate_cells = swap(mate_cells)

    line = [block]
    for shift in STEPS:
        line.append(send(block, along(True, shift)))
    group = jnp.concatenate(line, axis=0)
    gathered = [group]
    for shift in STEPS:
        gathered.append(send(group, along(False, shift)))

    grown, tall = ((6144, 128), F32), ((128, 1024), F32)
    spread = ((128, 1024), BF)
    table, wide, mixed, gain = call(
        table_kernel,
        [((4096, 128), F32), spread, spread, ((1, 1024), F32)],
        [tall],
        2_000_000_000,
        12,
        3,
    )(cells, w_in, ln_gain[None])
    picked = ((16, 128, 128), F32)
    edge, table = call(
        encode_edge_kernel, [((256, 128), BF), grown], [tall, picked], 3_000_000_000, 8, 4, 1
    )(cell_index, interp_weight, near_cells, mate_cells, table)
    near = neighbour(edge)
    (inner,) = call(
        encode_inner_kernel, [((256, 128), BF)], [picked], 3_000_000_000, 8, 2, 1
    )(cell_index, interp_weight, table)
    packed = jnp.concatenate([edge, inner, near], axis=0)
    mate = swap(packed)

    tile = ((512, 1024), BF)
    own, latent = call(embed_own_kernel, [tile, tile], [], 1_500_000_000, 12, 4)(
        packed, wide, mixed, gain
    )
    (rest,) = call(
        embed_rest_kernel, [((1024, 1024), BF)], [], 3_000_000_000, 12, 4
    )(packed, mate, mixed, gain)
    *sums, latent = call(
        first_kernel,
        [((512, 1536), F32), ((512, 1536), F32), ((512, 1024), F32), tile],
        [pltpu.SemaphoreType.DMA],
        6_000_000_000,
        12,
        6,
        any_out=(3,),
    )(latent, own, rest, *gathered[:3])
    q, k, v = call(
        project_kernel, [((4, n, 128), BF) for n in (1024, 1536, 1536)], [], 3_000_000_000, 12, 6
    )(own, rest, gathered[3], *sums)

    def attend(other, *args):
        kernel = functools.partial(attend_kernel, other)
        outs = [((12 if other else 4, 512, 128), BF)]
        return call(kernel, outs, [], 8_000_000_000, 16, len(args))(*args)[0]

    sent = attend(True, q, k, v, *gathered)
    theirs = swap(sent)
    mine = attend(False, q, k, v)
    (update,) = call(
        out_kernel,
        [tile],
        [tile, pltpu.SemaphoreType.DMA((2,))],
        1_000_000_000,
        12,
        3,
        any_out=(0,),
    )(mine, sent, theirs)
    return latent[None], update[None]


def solution(mesh):
    placed = (
        P("dp", None, "space"),
        P("space", None),
        P("space", None, None),
        P(),
        P(),
        P("dp", None),
        P("dp", None),
    )
    return jax.shard_map(
        shards,
        mesh=mesh,
        in_specs=placed,
        out_specs=(P("dp", "space", None), P("dp", "space", None)),
        check_vma=False,
    )
```
